32 devices in a mesh: dp: 2 (over x), tp: 4 (over z), ctx: 4 (over y, core).
Axes of the slice: x: 2, y: 2, z: 4, core: 2. Of those that a mesh axis runs over, the one named last changes fastest.
Arguments:
- x_tokens: bfloat16 [2048, 5120], P(('dp', 'ctx')), parts along dimension 0
- positions: int32 [2048], P(('dp', 'ctx')), parts along dimension 0
- w_dq: bfloat16 [5120, 1536], replicated
- g_q: bfloat16 [1536], replicated
- w_uq: bfloat16 [1536, 16384], P(None, 'tp')
- w_qr: bfloat16 [1536, 8192], P(None, 'tp')
- w_dkv: bfloat16 [5120, 512], replicated
- g_kv: bfloat16 [512], replicated
- w_kr: bfloat16 [5120, 64], replicated
- w_uk: bfloat16 [512, 16384], P(None, 'tp')
- w_uv: bfloat16 [512, 16384], P(None, 'tp')
- w_o: bfloat16 [16384, 5120], P('tp')
Outputs:
- output: bfloat16 [2048, 5120], P(('dp', 'ctx')), parts along dimension 0
There are 2 independent parts. The reference program is written for one: setup_inputs(seed, part) draws one part's arguments, and reference() takes and returns one part's arrays. A program takes and returns all parts, laid end to end along the dimension named above; an argument that names none is the same for every part.
All inputs are finite; a program needn't handle non-finite values.
Results may differ from the reference program's by a relative error of at most 0.00853476.
Values are sent between devices in bfloat16 or wider.
A program may use at most 1 GiB of HBM per device.

```python
import jax
import jax.numpy as jnp
from jax import lax

MODEL_DIM = 5120
NUM_HEADS = 128
QUERY_RANK = 1536
LATENT_RANK = 512
NOPE_DIM = 128
ROPE_DIM = 64
VALUE_DIM = 128
CTX_SIZE = 4
SEQ_LEN = 1024
QUERY_BLOCK = 64
PIECE_LEN = SEQ_LEN // (2 * CTX_SIZE)
ROPE_BASE = 10000.0
NORM_EPS = 1e-6


def draw_weight(key, fan_in, fan_out, gain):
    return (jax.random.normal(key, (fan_in, fan_out), jnp.float32) * gain).astype(jnp.bfloat16)


def draw_positions(pos_key):
    step_key, start_key = jax.random.split(pos_key)
    pos_steps = jax.random.randint(step_key, (SEQ_LEN,), 1, 3, jnp.int32)
    pos_start = jax.random.randint(start_key, (), 0, SEQ_LEN, jnp.int32)
    logical = (pos_start + jnp.cumsum(pos_steps)).astype(jnp.int32)
    pos_pieces = logical.reshape(2 * CTX_SIZE, PIECE_LEN)
    stored = jnp.stack([pos_pieces[:CTX_SIZE], pos_pieces[CTX_SIZE:][::-1]], axis=1)
    return stored.reshape(SEQ_LEN)


def setup_inputs(seed: int = 0, part: int = 0) -> dict:
    base_key = jax.random.key(seed)
    weight_keys = jax.random.split(base_key, 10)
    part_key = jax.random.fold_in(base_key, part)
    tok_key, pos_key = jax.random.split(part_key)
    x_tokens = jax.random.normal(tok_key, (SEQ_LEN, MODEL_DIM), jnp.float32).astype(jnp.bfloat16)
    out_gain = (NUM_HEADS * VALUE_DIM) ** -0.5 * SEQ_LEN ** 0.25
    return {
        'x_tokens': x_tokens,
        'positions': draw_positions(pos_key),
        'w_dq': draw_weight(weight_keys[0], MODEL_DIM, QUERY_RANK, MODEL_DIM ** -0.5),
        'g_q': jax.random.uniform(weight_keys[1], (QUERY_RANK,), jnp.float32, 0.5, 1.5).astype(jnp.bfloat16),
        'w_uq': draw_weight(weight_keys[2], QUERY_RANK, NUM_HEADS * NOPE_DIM, QUERY_RANK ** -0.5),
        'w_qr': draw_weight(weight_keys[3], QUERY_RANK, NUM_HEADS * ROPE_DIM, QUERY_RANK ** -0.5),
        'w_dkv': draw_weight(weight_keys[4], MODEL_DIM, LATENT_RANK, MODEL_DIM ** -0.5),
        'g_kv': jax.random.uniform(weight_keys[5], (LATENT_RANK,), jnp.float32, 0.5, 1.5).astype(jnp.bfloat16),
        'w_kr': draw_weight(weight_keys[6], MODEL_DIM, ROPE_DIM, MODEL_DIM ** -0.5),
        'w_uk': draw_weight(weight_keys[7], LATENT_RANK, NUM_HEADS * NOPE_DIM, LATENT_RANK ** -0.5),
        'w_uv': draw_weight(weight_keys[8], LATENT_RANK, NUM_HEADS * VALUE_DIM, LATENT_RANK ** -0.5),
        'w_o': draw_weight(weight_keys[9], NUM_HEADS * VALUE_DIM, MODEL_DIM, out_gain),
    }


def rms_norm(act_in, gain_vec):
    inv_rms = lax.rsqrt(jnp.mean(act_in * act_in, axis=-1, keepdims=True) + NORM_EPS)
    return act_in * inv_rms * gain_vec.astype(jnp.float32)


def rope_tables(pos_vals):
    half_dim = ROPE_DIM // 2
    inv_freq = ROPE_BASE ** (-jnp.arange(half_dim, dtype=jnp.float32) * 2.0 / ROPE_DIM)
    angles = pos_vals.astype(jnp.float32)[..., None] * inv_freq
    return jnp.cos(angles), jnp.sin(angles)


def apply_rope(act_in, cos_t, sin_t):
    half_dim = act_in.shape[-1] // 2
    first_half = act_in[..., :half_dim]
    second_half = act_in[..., half_dim:]
    return jnp.concatenate([first_half * cos_t - second_half * sin_t, second_half * cos_t + first_half * sin_t], axis=-1)


def reference(x_tokens, positions, w_dq, g_q, w_uq, w_qr, w_dkv, g_kv, w_kr, w_uk, w_uv, w_o):
    cos_t, sin_t = rope_tables(positions)
    c_q = rms_norm(jnp.dot(x_tokens, w_dq, preferred_element_type=jnp.float32), g_q).astype(jnp.bfloat16)
    q_nope = jnp.dot(c_q, w_uq, preferred_element_type=jnp.float32).astype(jnp.bfloat16)
    q_rot = jnp.dot(c_q, w_qr, preferred_element_type=jnp.float32).reshape(SEQ_LEN, NUM_HEADS, ROPE_DIM)
    q_pe = apply_rope(q_rot, cos_t[:, None, :], sin_t[:, None, :]).astype(jnp.bfloat16)
    c_kv = rms_norm(jnp.dot(x_tokens, w_dkv, preferred_element_type=jnp.float32), g_kv).astype(jnp.bfloat16)
    k_pe = apply_rope(jnp.dot(x_tokens, w_kr, preferred_element_type=jnp.float32), cos_t, sin_t).astype(jnp.bfloat16).astype(jnp.float32)
    k_nope = jnp.dot(c_kv, w_uk, preferred_element_type=jnp.float32).astype(jnp.bfloat16).astype(jnp.float32).reshape(SEQ_LEN, NUM_HEADS, NOPE_DIM)
    values = jnp.dot(c_kv, w_uv, preferred_element_type=jnp.float32).astype(jnp.bfloat16).astype(jnp.float32).reshape(SEQ_LEN, NUM_HEADS, VALUE_DIM)
    score_scale = (NOPE_DIM + ROPE_DIM) ** -0.5
    block_count = SEQ_LEN // QUERY_BLOCK

    def attend_block(q_block):
        qn_blk, qp_blk, qpos_blk = q_block
        scores = jnp.einsum('qhn,khn->hqk', qn_blk.astype(jnp.float32), k_nope) + jnp.einsum('qhr,kr->hqk', qp_blk.astype(jnp.float32), k_pe)
        visible = positions[None, None, :] <= qpos_blk[None, :, None]
        scores = jnp.where(visible, scores * score_scale, -jnp.inf)
        prob_tile = jax.nn.softmax(scores, axis=-1)
        return jnp.einsum('hqk,khv->qhv', prob_tile, values).astype(jnp.bfloat16)

    attn_out = lax.map(attend_block, (q_nope.reshape(block_count, QUERY_BLOCK, NUM_HEADS, NOPE_DIM), q_pe.reshape(block_count, QUERY_BLOCK, NUM_HEADS, ROPE_DIM), positions.reshape(block_count, QUERY_BLOCK)))
    attn_out = attn_out.reshape(SEQ_LEN, NUM_HEADS * VALUE_DIM)
    return jnp.dot(attn_out, w_o, preferred_element_type=jnp.float32).astype(jnp.bfloat16)
```

```python
import jax
import jax.numpy as jnp
from jax import lax
from jax.experimental import pallas as pl
from jax.experimental.pallas import tpu as pltpu
from jax.sharding import PartitionSpec as P

ROPE_BASE = 10000.0
NORM_EPS = 1e-6
NEG_BIG = -1e30


def rms_norm(act_in, gain_vec):
    inv_rms = lax.rsqrt(jnp.mean(act_in * act_in, axis=-1, keepdims=True) + NORM_EPS)
    return act_in * inv_rms * gain_vec.astype(jnp.float32)


def rope_tables(pos_vals, rope_dim):
    half_dim = rope_dim // 2
    inv_freq = ROPE_BASE ** (-jnp.arange(half_dim, dtype=jnp.float32) * 2.0 / rope_dim)
    angles = pos_vals.astype(jnp.float32)[..., None] * inv_freq
    return jnp.cos(angles), jnp.sin(angles)


def apply_rope(act_in, cos_t, sin_t):
    half_dim = act_in.shape[-1] // 2
    first_half = act_in[..., :half_dim]
    second_half = act_in[..., half_dim:]
    return jnp.concatenate([first_half * cos_t - second_half * sin_t, second_half * cos_t + first_half * sin_t], axis=-1)


def project_tokens(tok_x, tok_pos, w_dq, g_q, w_uq, w_qr, w_dkv, g_kv, w_kr, heads_loc):
    rope_dim = w_kr.shape[1]
    tok_count = tok_x.shape[0]
    cos_t, sin_t = rope_tables(tok_pos, rope_dim)
    c_q = rms_norm(jnp.dot(tok_x, w_dq, preferred_element_type=jnp.float32), g_q).astype(jnp.bfloat16)
    q_nope = jnp.dot(c_q, w_uq, preferred_element_type=jnp.float32).astype(jnp.bfloat16).reshape(tok_count, heads_loc, -1)
    q_rot = jnp.dot(c_q, w_qr, preferred_element_type=jnp.float32).reshape(tok_count, heads_loc, rope_dim)
    q_pe = apply_rope(q_rot, cos_t[:, None, :], sin_t[:, None, :]).astype(jnp.bfloat16)
    c_kv = rms_norm(jnp.dot(tok_x, w_dkv, preferred_element_type=jnp.float32), g_kv).astype(jnp.bfloat16)
    k_pe = apply_rope(jnp.dot(tok_x, w_kr, preferred_element_type=jnp.float32), cos_t, sin_t).astype(jnp.bfloat16)
    return q_nope, q_pe, c_kv, k_pe


def up_project(lat_rows, w_uk, w_uv, heads_loc):
    row_count = lat_rows.shape[0]
    k_nope = jnp.dot(lat_rows, w_uk, preferred_element_type=jnp.float32).astype(jnp.bfloat16).reshape(row_count, heads_loc, -1)
    v_rows = jnp.dot(lat_rows, w_uv, preferred_element_type=jnp.float32).astype(jnp.bfloat16).reshape(row_count, heads_loc, -1)
    return k_nope, v_rows


def block_scores(q_nope, q_pe, k_nope, k_pe, score_scale):
    nope_part = jnp.einsum('qhn,khn->hqk', q_nope, k_nope, preferred_element_type=jnp.float32)
    rope_part = jnp.einsum('qhr,kr->hqk', q_pe, k_pe, preferred_element_type=jnp.float32)
    return (nope_part + rope_part) * score_scale


def block_stats(scores, v_rows):
    blk_max = jnp.max(scores, axis=-1)
    prob_tile = jnp.exp(scores - blk_max[..., None])
    blk_sum = jnp.sum(prob_tile, axis=-1)
    blk_acc = jnp.einsum('hqk,khv->hqv', prob_tile.astype(jnp.bfloat16), v_rows, preferred_element_type=jnp.float32)
    return blk_max, blk_sum, blk_acc


def merge_stats(run_state, update):
    old_max, old_sum, old_acc = run_state
    new_max, new_sum, new_acc = update
    top_max = jnp.maximum(old_max, new_max)
    old_w = jnp.exp(old_max - top_max)
    new_w = jnp.exp(new_max - top_max)
    return top_max, old_sum * old_w + new_sum * new_w, old_acc * old_w[..., None] + new_acc * new_w[..., None]


TP = 4
ROW_BLK = 128
COL_BLK = 256
SLOTS = 3
FIRST_EVENT = 3


def out_sum_kernel(o_ref, w_hbm, y_ref, acc, rbuf, wbuf, w_sem, f_send, f_recv, b_send, b_recv):
    my_tp = lax.axis_index('tp')
    n_rows, n_cols = y_ref.shape
    row_blks = n_rows // ROW_BLK
    half_cols = n_cols // 2
    col_steps = half_cols // COL_BLK
    n_chunks = col_steps * row_blks
    left = lax.rem(my_tp + TP - 1, TP)
    right = lax.rem(my_tp + 1, TP)
    depth = (TP - 1 - my_tp, my_tp)
    onward = (left, right)
    back = (right, left)

    def w_copy(step, side):
        slot = lax.rem(step, SLOTS)
        cols = pl.ds(pl.multiple_of(side * half_cols + step * COL_BLK, COL_BLK), COL_BLK)
        return pltpu.make_async_copy(w_hbm.at[:, cols], wbuf.at[slot, side], w_sem.at[slot, side])

    def y_slice(side, chunk):
        step, row = chunk // row_blks, lax.rem(chunk, row_blks)
        return (pl.ds(pl.multiple_of(row * ROW_BLK, ROW_BLK), ROW_BLK),
                pl.ds(pl.multiple_of(side * half_cols + step * COL_BLK, COL_BLK), COL_BLK))

    def f_copy(side, chunk):
        return pltpu.make_async_remote_copy(
            src_ref=acc.at[side, chunk], dst_ref=rbuf.at[side, chunk],
            send_sem=f_send.at[side, chunk], recv_sem=f_recv.at[side, chunk],
            device_id={'tp': onward[side]}, device_id_type=pl.DeviceIdType.MESH)

    def b_copy(side, chunk):
        part = y_ref.at[y_slice(side, chunk)]
        return pltpu.make_async_remote_copy(
            src_ref=part, dst_ref=part,
            send_sem=b_send.at[side, chunk], recv_sem=b_recv.at[side, chunk],
            device_id={'tp': back[side]}, device_id_type=pl.DeviceIdType.MESH)

    for pre in range(SLOTS - 1):
        for side in range(2):
            w_copy(pre, side).start()

    barrier = pltpu.get_barrier_semaphore()

    @pl.when(my_tp > 0)
    def _():
        pl.semaphore_signal(barrier, inc=1, device_id={'tp': left}, device_id_type=pl.DeviceIdType.MESH)

    @pl.when(my_tp < TP - 1)
    def _():
        pl.semaphore_signal(barrier, inc=1, device_id={'tp': right}, device_id_type=pl.DeviceIdType.MESH)

    @pl.when((my_tp > 0) & (my_tp < TP - 1))
    def _():
        pl.semaphore_wait(barrier, 2)

    @pl.when((my_tp == 0) | (my_tp == TP - 1))
    def _():
        pl.semaphore_wait(barrier, 1)

    def reduce_event(side, chunk):
        @pl.when(depth[side] > 0)
        def _():
            f_copy(side, chunk).wait_recv()

        @pl.when((depth[side] > 0) & (depth[side] < TP - 1))
        def _():
            acc[side, chunk] = acc[side, chunk] + rbuf[side, chunk]
            f_copy(side, chunk).start()

        @pl.when(depth[side] == TP - 1)
        def _():
            total = acc[side, chunk] + rbuf[side, chunk]
            y_ref[y_slice(side, chunk)] = total.astype(y_ref.dtype)
            b_copy(side, chunk).start()

    def compute_step(step, _):
        slot = lax.rem(step, SLOTS)

        @pl.when(step + SLOTS - 1 < col_steps)
        def _():
            for side in range(2):
                w_copy(step + SLOTS - 1, side).start()

        for side in range(2):
            w_copy(step, side).wait()
            part = jnp.dot(o_ref[...], wbuf[slot, side], preferred_element_type=jnp.float32)
            for row in range(row_blks):
                chunk = step * row_blks + row
                acc[side, chunk] = part[row * ROW_BLK:(row + 1) * ROW_BLK]

                @pl.when(depth[side] == 0)
                def _():
                    f_copy(side, chunk).start()

        @pl.when(step >= FIRST_EVENT)
        def _():
            for side in range(2):
                reduce_event(side, step - FIRST_EVENT)
        return 0

    lax.fori_loop(0, col_steps, compute_step, 0)

    def late_event(chunk, _):
        for side in range(2):
            reduce_event(side, chunk)
        return 0

    lax.fori_loop(col_steps - FIRST_EVENT, n_chunks, late_event, 0)

    def back_event(chunk, _):
        for side in range(2):
            @pl.when(depth[side] < TP - 1)
            def _():
                b_copy(side, chunk).wait_recv()

            @pl.when((depth[side] > 0) & (depth[side] < TP - 1))
            def _():
                b_copy(side, chunk).start()
        return 0

    lax.fori_loop(0, n_chunks, back_event, 0)

    def drain(chunk, _):
        for side in range(2):
            @pl.when(depth[side] < TP - 1)
            def _():
                f_copy(side, chunk).wait_send()

            @pl.when(depth[side] > 0)
            def _():
                b_copy(side, chunk).wait_send()
        return 0

    lax.fori_loop(0, n_chunks, drain, 0)


def out_sum(attn_out, w_o):
    n_rows, n_depth = attn_out.shape
    n_cols = w_o.shape[1]
    n_chunks = (n_cols // 2 // COL_BLK) * (n_rows // ROW_BLK)
    return pl.pallas_call(
        out_sum_kernel,
        out_shape=jax.ShapeDtypeStruct((n_rows, n_cols), jnp.bfloat16),
        in_specs=[pl.BlockSpec(memory_space=pltpu.VMEM), pl.BlockSpec(memory_space=pl.ANY)],
        out_specs=pl.BlockSpec(memory_space=pltpu.VMEM),
        scratch_shapes=[
            pltpu.VMEM((2, n_chunks, ROW_BLK, COL_BLK), jnp.float32),
            pltpu.VMEM((2, n_chunks, ROW_BLK, COL_BLK), jnp.float32),
            pltpu.VMEM((SLOTS, 2, n_depth, COL_BLK), jnp.bfloat16),
            pltpu.SemaphoreType.DMA((SLOTS, 2)),
            pltpu.SemaphoreType.DMA((2, n_chunks)),
            pltpu.SemaphoreType.DMA((2, n_chunks)),
            pltpu.SemaphoreType.DMA((2, n_chunks)),
            pltpu.SemaphoreType.DMA((2, n_chunks)),
        ],
        compiler_params=pltpu.CompilerParams(collective_id=0, has_side_effects=True, vmem_limit_bytes=50 * 2 ** 20),
        name='out_sum',
    )(attn_out, w_o)


def solution(mesh):
    ctx_count = mesh.shape['ctx']
    next_perm = [(src, (src + 1) % ctx_count) for src in range(ctx_count)]
    tok_spec = P(('dp', 'ctx'), None)
    pos_spec = P(('dp', 'ctx'))
    full_mat = P(None, None)
    full_vec = P(None)
    col_spec = P(None, 'tp')
    row_spec = P('tp', None)

    def local_step(tok_x, tok_pos, w_dq, g_q, w_uq, w_qr, w_dkv, g_kv, w_kr, w_uk, w_uv, w_o):
        my_index = lax.axis_index('ctx')
        half_len = tok_x.shape[0] // 2
        rope_dim = w_kr.shape[1]
        heads_loc = w_qr.shape[1] // rope_dim
        nope_dim = w_uq.shape[1] // heads_loc
        value_dim = w_uv.shape[1] // heads_loc
        score_scale = (nope_dim + rope_dim) ** -0.5
        q_nope, q_pe, c_kv, k_pe = project_tokens(tok_x, tok_pos, w_dq, g_q, w_uq, w_qr, w_dkv, g_kv, w_kr, heads_loc)
        k_nope, v_rows = up_project(c_kv, w_uk, w_uv, heads_loc)
        scores = block_scores(q_nope, q_pe, k_nope, k_pe, score_scale)
        visible = tok_pos[None, :] <= tok_pos[:, None]
        run_state = block_stats(jnp.where(visible[None], scores, NEG_BIG), v_rows)

        def attend_lower(lat_blk, rot_blk, run_state):
            k_low, v_low = up_project(lat_blk[:half_len], w_uk, w_uv, heads_loc)
            update = block_stats(block_scores(q_nope, q_pe, k_low, rot_blk[:half_len], score_scale), v_low)
            return merge_stats(run_state, update)

        def attend_upper(lat_blk, rot_blk, run_state):
            k_both, v_both = up_project(lat_blk, w_uk, w_uv, heads_loc)
            update = block_stats(block_scores(q_nope[half_len:], q_pe[half_len:], k_both, rot_blk, score_scale), v_both)
            old_max, old_sum, old_acc = run_state
            top_max, top_sum, top_acc = merge_stats((old_max[:, half_len:], old_sum[:, half_len:], old_acc[:, half_len:]), update)
            return (jnp.concatenate([old_max[:, :half_len], top_max], axis=1),
                    jnp.concatenate([old_sum[:, :half_len], top_sum], axis=1),
                    jnp.concatenate([old_acc[:, :half_len], top_acc], axis=1))

        def ctx_step(hop_idx, loop_carry):
            lat_blk, rot_blk, run_state = loop_carry
            lat_blk = lax.ppermute(lat_blk, 'ctx', next_perm)
            rot_blk = lax.ppermute(rot_blk, 'ctx', next_perm)
            src_index = (my_index - hop_idx) % ctx_count
            run_state = lax.cond(src_index < my_index, attend_lower, attend_upper, lat_blk, rot_blk, run_state)
            return lat_blk, rot_blk, run_state

        loop_carry = lax.fori_loop(1, ctx_count, ctx_step, (c_kv, k_pe, run_state))
        run_max, run_sum, run_acc = loop_carry[2]
        attn_out = (run_acc / run_sum[..., None]).astype(jnp.bfloat16)
        attn_rows = attn_out.transpose(1, 0, 2).reshape(tok_x.shape[0], heads_loc * value_dim)
        return out_sum(attn_rows, w_o)

    return jax.shard_map(local_step, mesh=mesh,
                         in_specs=(tok_spec, pos_spec, full_mat, full_vec, col_spec, col_spec, full_mat, full_vec, full_mat, col_spec, col_spec, row_spec),
                         out_specs=tok_spec, check_vma=False)
```

```python
import jax
import jax.numpy as jnp
from jax import lax
from jax.experimental import pallas as pl
from jax.experimental.pallas import tpu as pltpu
from jax.sharding import PartitionSpec as P

ROPE_BASE = 10000.0
NORM_EPS = 1e-6
NEG_BIG = -1e30


def rms_norm(act_in, gain_vec):
    inv_rms = lax.rsqrt(jnp.mean(act_in * act_in, axis=-1, keepdims=True) + NORM_EPS)
    return act_in * inv_rms * gain_vec.astype(jnp.float32)


def rope_tables(pos_vals, rope_dim):
    half_dim = rope_dim // 2
    inv_freq = ROPE_BASE ** (-jnp.arange(half_dim, dtype=jnp.float32) * 2.0 / rope_dim)
    angles = pos_vals.astype(jnp.float32)[..., None] * inv_freq
    return jnp.cos(angles), jnp.sin(angles)


def apply_rope(act_in, cos_t, sin_t):
    half_dim = act_in.shape[-1] // 2
    first_half = act_in[..., :half_dim]
    second_half = act_in[..., half_dim:]
    return jnp.concatenate([first_half * cos_t - second_half * sin_t, second_half * cos_t + first_half * sin_t], axis=-1)


def project_tokens(tok_x, tok_pos, w_dq, g_q, w_uq, w_qr, w_dkv, g_kv, w_kr, heads_loc):
    rope_dim = w_kr.shape[1]
    tok_count = tok_x.shape[0]
    cos_t, sin_t = rope_tables(tok_pos, rope_dim)
    c_q = rms_norm(jnp.dot(tok_x, w_dq, preferred_element_type=jnp.float32), g_q).astype(jnp.bfloat16)
    q_nope = jnp.dot(c_q, w_uq, preferred_element_type=jnp.float32).astype(jnp.bfloat16).reshape(tok_count, heads_loc, -1)
    q_rot = jnp.dot(c_q, w_qr, preferred_element_type=jnp.float32).reshape(tok_count, heads_loc, rope_dim)
    q_pe = apply_rope(q_rot, cos_t[:, None, :], sin_t[:, None, :]).astype(jnp.bfloat16)
    c_kv = rms_norm(jnp.dot(tok_x, w_dkv, preferred_element_type=jnp.float32), g_kv).astype(jnp.bfloat16)
    k_pe = apply_rope(jnp.dot(tok_x, w_kr, preferred_element_type=jnp.float32), cos_t, sin_t).astype(jnp.bfloat16)
    return q_nope, q_pe, c_kv, k_pe


def up_project(lat_rows, w_uk, w_uv, heads_loc):
    row_count = lat_rows.shape[0]
    k_nope = jnp.dot(lat_rows, w_uk, preferred_element_type=jnp.float32).astype(jnp.bfloat16).reshape(row_count, heads_loc, -1)
    v_rows = jnp.dot(lat_rows, w_uv, preferred_element_type=jnp.float32).astype(jnp.bfloat16).reshape(row_count, heads_loc, -1)
    return k_nope, v_rows


def block_scores(q_nope, q_pe, k_nope, k_pe, score_scale):
    nope_part = jnp.einsum('qhn,khn->hqk', q_nope, k_nope, preferred_element_type=jnp.float32)
    rope_part = jnp.einsum('qhr,kr->hqk', q_pe, k_pe, preferred_element_type=jnp.float32)
    return (nope_part + rope_part) * score_scale


def block_stats(scores, v_rows):
    blk_max = jnp.max(scores, axis=-1)
    prob_tile = jnp.exp(scores - blk_max[..., None])
    blk_sum = jnp.sum(prob_tile, axis=-1)
    blk_acc = jnp.einsum('hqk,khv->hqv', prob_tile.astype(jnp.bfloat16), v_rows, preferred_element_type=jnp.float32)
    return blk_max, blk_sum, blk_acc


def merge_stats(run_state, update):
    old_max, old_sum, old_acc = run_state
    new_max, new_sum, new_acc = update
    top_max = jnp.maximum(old_max, new_max)
    old_w = jnp.exp(old_max - top_max)
    new_w = jnp.exp(new_max - top_max)
    return top_max, old_sum * old_w + new_sum * new_w, old_acc * old_w[..., None] + new_acc * new_w[..., None]


TP = 4
ROW_BLK = 128
COL_BLK = 256
SLOTS = 3
FIRST_EVENT = 3
SUM_LAG = 2
BACK_LAG = 3


def out_sum_kernel(o_ref, w_hbm, y_ref, acc, rbuf, wbuf, w_sem, f_send, f_recv, b_send, b_recv):
    my_tp = lax.axis_index('tp')
    n_rows, n_cols = y_ref.shape
    row_blks = n_rows // ROW_BLK
    half_cols = n_cols // 2
    col_steps = half_cols // COL_BLK
    n_chunks = col_steps * row_blks
    left = lax.rem(my_tp + TP - 1, TP)
    right = lax.rem(my_tp + 1, TP)
    depth = (TP - 1 - my_tp, my_tp)
    onward = (left, right)
    back = (right, left)

    def w_copy(step, side):
        slot = lax.rem(step, SLOTS)
        cols = pl.ds(pl.multiple_of(side * half_cols + step * COL_BLK, COL_BLK), COL_BLK)
        return pltpu.make_async_copy(w_hbm.at[:, cols], wbuf.at[slot, side], w_sem.at[slot, side])

    def y_slice(side, chunk):
        step, row = chunk // row_blks, lax.rem(chunk, row_blks)
        return (pl.ds(pl.multiple_of(row * ROW_BLK, ROW_BLK), ROW_BLK),
                pl.ds(pl.multiple_of(side * half_cols + step * COL_BLK, COL_BLK), COL_BLK))

    def f_copy(side, chunk):
        return pltpu.make_async_remote_copy(
            src_ref=acc.at[side, chunk], dst_ref=rbuf.at[side, chunk],
            send_sem=f_send.at[side, chunk], recv_sem=f_recv.at[side, chunk],
            device_id={'tp': onward[side]}, device_id_type=pl.DeviceIdType.MESH)

    def b_copy(side, chunk):
        part = y_ref.at[y_slice(side, chunk)]
        return pltpu.make_async_remote_copy(
            src_ref=part, dst_ref=part,
            send_sem=b_send.at[side, chunk], recv_sem=b_recv.at[side, chunk],
            device_id={'tp': back[side]}, device_id_type=pl.DeviceIdType.MESH)

    for pre in range(SLOTS - 1):
        for side in range(2):
            w_copy(pre, side).start()

    barrier = pltpu.get_barrier_semaphore()

    @pl.when(my_tp > 0)
    def _():
        pl.semaphore_signal(barrier, inc=1, device_id={'tp': left}, device_id_type=pl.DeviceIdType.MESH)

    @pl.when(my_tp < TP - 1)
    def _():
        pl.semaphore_signal(barrier, inc=1, device_id={'tp': right}, device_id_type=pl.DeviceIdType.MESH)

    @pl.when((my_tp > 0) & (my_tp < TP - 1))
    def _():
        pl.semaphore_wait(barrier, 2)

    @pl.when((my_tp == 0) | (my_tp == TP - 1))
    def _():
        pl.semaphore_wait(barrier, 1)

    def reduce_event(side, event):
        chunk = event - SUM_LAG * (depth[side] - 1)
        live = (chunk >= 0) & (chunk < n_chunks)

        @pl.when(live & (depth[side] > 0))
        def _():
            f_copy(side, chunk).wait_recv()

        @pl.when(live & (depth[side] > 0) & (depth[side] < TP - 1))
        def _():
            acc[side, chunk] = acc[side, chunk] + rbuf[side, chunk]
            f_copy(side, chunk).start()

        @pl.when(live & (depth[side] == TP - 1))
        def _():
            total = acc[side, chunk] + rbuf[side, chunk]
            y_ref[y_slice(side, chunk)] = total.astype(y_ref.dtype)
            b_copy(side, chunk).start()

    def compute_step(step, _):
        slot = lax.rem(step, SLOTS)

        @pl.when(step + SLOTS - 1 < col_steps)
        def _():
            for side in range(2):
                w_copy(step + SLOTS - 1, side).start()

        for side in range(2):
            w_copy(step, side).wait()
            part = jnp.dot(o_ref[...], wbuf[slot, side], preferred_element_type=jnp.float32)
            for row in range(row_blks):
                chunk = step * row_blks + row
                acc[side, chunk] = part[row * ROW_BLK:(row + 1) * ROW_BLK]

                @pl.when(depth[side] == 0)
                def _():
                    f_copy(side, chunk).start()

        @pl.when(step >= FIRST_EVENT)
        def _():
            for side in range(2):
                reduce_event(side, step - FIRST_EVENT)
        return 0

    lax.fori_loop(0, col_steps, compute_step, 0)

    def late_event(event, _):
        for side in range(2):
            reduce_event(side, event)
        return 0

    lax.fori_loop(col_steps - FIRST_EVENT, n_chunks + SUM_LAG * (TP - 2), late_event, 0)

    def back_event(event, _):
        for side in range(2):
            chunk = event - BACK_LAG * (TP - 2 - depth[side])
            live = (chunk >= 0) & (chunk < n_chunks)

            @pl.when(live & (depth[side] < TP - 1))
            def _():
                b_copy(side, chunk).wait_recv()

            @pl.when(live & (depth[side] > 0) & (depth[side] < TP - 1))
            def _():
                b_copy(side, chunk).start()
        return 0

    lax.fori_loop(0, n_chunks + BACK_LAG * (TP - 2), back_event, 0)

    def drain(chunk, _):
        for side in range(2):
            @pl.when(depth[side] < TP - 1)
            def _():
                f_copy(side, chunk).wait_send()

            @pl.when(depth[side] > 0)
            def _():
                b_copy(side, chunk).wait_send()
        return 0

    lax.fori_loop(0, n_chunks, drain, 0)


def out_sum(attn_out, w_o):
    n_rows, n_depth = attn_out.shape
    n_cols = w_o.shape[1]
    n_chunks = (n_cols // 2 // COL_BLK) * (n_rows // ROW_BLK)
    return pl.pallas_call(
        out_sum_kernel,
        out_shape=jax.ShapeDtypeStruct((n_rows, n_cols), jnp.bfloat16),
        in_specs=[pl.BlockSpec(memory_space=pltpu.VMEM), pl.BlockSpec(memory_space=pl.ANY)],
        out_specs=pl.BlockSpec(memory_space=pltpu.VMEM),
        scratch_shapes=[
            pltpu.VMEM((2, n_chunks, ROW_BLK, COL_BLK), jnp.float32),
            pltpu.VMEM((2, n_chunks, ROW_BLK, COL_BLK), jnp.float32),
            pltpu.VMEM((SLOTS, 2, n_depth, COL_BLK), jnp.bfloat16),
            pltpu.SemaphoreType.DMA((SLOTS, 2)),
            pltpu.SemaphoreType.DMA((2, n_chunks)),
            pltpu.SemaphoreType.DMA((2, n_chunks)),
            pltpu.SemaphoreType.DMA((2, n_chunks)),
            pltpu.SemaphoreType.DMA((2, n_chunks)),
        ],
        compiler_params=pltpu.CompilerParams(collective_id=0, has_side_effects=True, vmem_limit_bytes=50 * 2 ** 20),
        name='out_sum',
    )(attn_out, w_o)


def solution(mesh):
    ctx_count = mesh.shape['ctx']
    next_perm = [(src, (src + 1) % ctx_count) for src in range(ctx_count)]
    tok_spec = P(('dp', 'ctx'), None)
    pos_spec = P(('dp', 'ctx'))
    full_mat = P(None, None)
    full_vec = P(None)
    col_spec = P(None, 'tp')
    row_spec = P('tp', None)

    def local_step(tok_x, tok_pos, w_dq, g_q, w_uq, w_qr, w_dkv, g_kv, w_kr, w_uk, w_uv, w_o):
        my_index = lax.axis_index('ctx')
        half_len = tok_x.shape[0] // 2
        rope_dim = w_kr.shape[1]
        heads_loc = w_qr.shape[1] // rope_dim
        nope_dim = w_uq.shape[1] // heads_loc
        value_dim = w_uv.shape[1] // heads_loc
        score_scale = (nope_dim + rope_dim) ** -0.5
        q_nope, q_pe, c_kv, k_pe = project_tokens(tok_x, tok_pos, w_dq, g_q, w_uq, w_qr, w_dkv, g_kv, w_kr, heads_loc)
        k_nope, v_rows = up_project(c_kv, w_uk, w_uv, heads_loc)
        scores = block_scores(q_nope, q_pe, k_nope, k_pe, score_scale)
        visible = tok_pos[None, :] <= tok_pos[:, None]
        run_state = block_stats(jnp.where(visible[None], scores, NEG_BIG), v_rows)

        def attend_lower(lat_blk, rot_blk, run_state):
            k_low, v_low = up_project(lat_blk[:half_len], w_uk, w_uv, heads_loc)
            update = block_stats(block_scores(q_nope, q_pe, k_low, rot_blk[:half_len], score_scale), v_low)
            return merge_stats(run_state, update)

        def attend_upper(lat_blk, rot_blk, run_state):
            k_both, v_both = up_project(lat_blk, w_uk, w_uv, heads_loc)
            update = block_stats(block_scores(q_nope[half_len:], q_pe[half_len:], k_both, rot_blk, score_scale), v_both)
            old_max, old_sum, old_acc = run_state
            top_max, top_sum, top_acc = merge_stats((old_max[:, half_len:], old_sum[:, half_len:], old_acc[:, half_len:]), update)
            return (jnp.concatenate([old_max[:, :half_len], top_max], axis=1),
                    jnp.concatenate([old_sum[:, :half_len], top_sum], axis=1),
                    jnp.concatenate([old_acc[:, :half_len], top_acc], axis=1))

        def ctx_step(hop_idx, loop_carry):
            lat_blk, rot_blk, run_state = loop_carry
            lat_blk = lax.ppermute(lat_blk, 'ctx', next_perm)
            rot_blk = lax.ppermute(rot_blk, 'ctx', next_perm)
            src_index = (my_index - hop_idx) % ctx_count
            run_state = lax.cond(src_index < my_index, attend_lower, attend_upper, lat_blk, rot_blk, run_state)
            return lat_blk, rot_blk, run_state

        loop_carry = lax.fori_loop(1, ctx_count, ctx_step, (c_kv, k_pe, run_state))
        run_max, run_sum, run_acc = loop_carry[2]
        attn_out = (run_acc / run_sum[..., None]).astype(jnp.bfloat16)
        attn_rows = attn_out.transpose(1, 0, 2).reshape(tok_x.shape[0], heads_loc * value_dim)
        return out_sum(attn_rows, w_o)

    return jax.shard_map(local_step, mesh=mesh,
                         in_specs=(tok_spec, pos_spec, full_mat, full_vec, col_spec, col_spec, full_mat, full_vec, full_mat, col_spec, col_spec, row_spec),
                         out_specs=tok_spec, check_vma=False)
```

```python
import math

import jax
import jax.numpy as jnp
from jax import lax
from jax.experimental import pallas as pl
from jax.experimental.pallas import tpu as pltpu
from jax.sharding import PartitionSpec as P

ROPE_BASE = 10000.0
NORM_EPS = 1e-6
NEG_BIG = -1e30
POS_BIG = 3e38
TP = 4
CTX = 4
PIECE = 128
NOPE = 128
ROPE = 64
VALUE = 128
GROUP = 4
DOWN_BLK = 512
COL_BLK = 256
O_SLOTS = 3
FIRST_EVENT = 3
SUM_LAG = 2
BACK_LAG = 3
RELAY_AT = 5
MESH_ID = pl.DeviceIdType.MESH


def rope_tables(pos_vals, copies):
    half_dim = ROPE // 2
    inv_freq = ROPE_BASE ** (-jnp.arange(half_dim, dtype=jnp.float32) * 2.0 / ROPE)
    angles = pos_vals.astype(jnp.float32)[..., None] * inv_freq
    cos_t, sin_t = jnp.cos(angles), jnp.sin(angles)
    return (jnp.concatenate([cos_t, cos_t] * copies, axis=-1),
            jnp.concatenate([-sin_t, sin_t] * copies, axis=-1))


def rms_norm(act_in, gain_row):
    inv_rms = lax.rsqrt(jnp.mean(act_in * act_in, axis=-1, keepdims=True) + NORM_EPS)
    return act_in * inv_rms * gain_row


def rotate(rows, cos_t, sin_t):
    width = rows.shape[1]
    lane = lax.broadcasted_iota(jnp.int32, rows.shape, 1)
    swapped = jnp.where(lax.rem(lane, ROPE) < ROPE // 2,
                        pltpu.roll(rows, width - ROPE // 2, 1), pltpu.roll(rows, ROPE // 2, 1))
    return rows * cos_t + swapped * sin_t


def layer_kernel(x_hbm, cos_ref, sin_ref, gq_ref, gkv_ref, wdq_hbm, wuq_hbm, wqr_hbm, wdkv_hbm, wkr_hbm, wuk_hbm, wuv_hbm, wo_hbm,
                 y_ref,
                 x_ref, wkr_ref, wdown, wq, wqr, wkv, wo,
                 lat, kpe, cq_f, cq, qn, qp, cap, o_ref, acc, rbuf,
                 x_sem, kr_sem, down_sem, q_sem, kv_sem, o_sem,
                 lat_send, lat_recv, f_send, f_recv, b_send, b_recv):
    my_tp = lax.axis_index('tp')
    my_ctx = lax.axis_index('ctx')
    n_rows, n_cols = y_ref.shape
    heads = o_ref.shape[1] // VALUE
    groups = heads // GROUP
    q_rank = cq.shape[1]
    lat_rank = wkv.shape[2]
    n_keys = 2 * CTX * PIECE
    low_keys = CTX * PIECE
    n_down = 1 + q_rank // DOWN_BLK
    left = lax.rem(my_tp + TP - 1, TP)
    right = lax.rem(my_tp + 1, TP)
    partner = my_ctx + 1 - 2 * lax.rem(my_ctx, 2)
    across = lax.rem(my_ctx + 2, CTX)

    x_copy = pltpu.make_async_copy(x_hbm, x_ref, x_sem)
    kr_copy = pltpu.make_async_copy(wkr_hbm, wkr_ref, kr_sem)

    def dq_copy(blk):
        cols = pl.ds(pl.multiple_of((blk - 1) * DOWN_BLK, DOWN_BLK), DOWN_BLK)
        slot = lax.rem(blk, 2)
        return pltpu.make_async_copy(wdq_hbm.at[:, cols], wdown.at[slot], down_sem.at[slot])

    dkv_copy = pltpu.make_async_copy(wdkv_hbm, wdown.at[0], down_sem.at[0])

    def q_copies(grp):
        slot = lax.rem(grp, 2)
        n_blk, r_blk = GROUP * NOPE, GROUP * ROPE
        return (pltpu.make_async_copy(wuq_hbm.at[:, pl.ds(pl.multiple_of(grp * n_blk, n_blk), n_blk)], wq.at[slot], q_sem.at[slot, 0]),
                pltpu.make_async_copy(wqr_hbm.at[:, pl.ds(pl.multiple_of(grp * r_blk, r_blk), r_blk)], wqr.at[slot], q_sem.at[slot, 1]))

    def kv_copies(grp):
        slot = lax.rem(grp, 2)
        n_blk = GROUP * NOPE
        cols = pl.ds(pl.multiple_of(grp * n_blk, n_blk), n_blk)
        return (pltpu.make_async_copy(wuk_hbm.at[:, cols], wkv.at[slot, 0], kv_sem.at[slot, 0]),
                pltpu.make_async_copy(wuv_hbm.at[:, cols], wkv.at[slot, 1], kv_sem.at[slot, 1]))

    row_blks = n_rows // PIECE
    half_cols = n_cols // 2
    col_steps = half_cols // COL_BLK
    n_chunks = col_steps * row_blks

    def o_copies(step):
        slot = lax.rem(step, O_SLOTS)
        return [pltpu.make_async_copy(
            wo_hbm.at[:, pl.ds(pl.multiple_of(side * half_cols + step * COL_BLK, COL_BLK), COL_BLK)],
            wo.at[slot, :, pl.ds(side * COL_BLK, COL_BLK)], o_sem.at[slot, side]) for side in range(2)]

    def start_all(copies):
        for copy in copies:
            copy.start()

    def wait_all(copies):
        for copy in copies:
            copy.wait()

    x_copy.start()
    kr_copy.start()
    dkv_copy.start()
    dq_copy(1).start()

    barrier = pltpu.get_barrier_semaphore()
    for peer in (partner, across):
        pl.semaphore_signal(barrier, inc=1, device_id={'ctx': peer}, device_id_type=MESH_ID)

    @pl.when(my_tp > 0)
    def _():
        pl.semaphore_signal(barrier, inc=1, device_id={'tp': left}, device_id_type=MESH_ID)

    @pl.when(my_tp < TP - 1)
    def _():
        pl.semaphore_signal(barrier, inc=1, device_id={'tp': right}, device_id_type=MESH_ID)

    for half, width in ((0, low_keys), (1, n_keys)):
        q_rank_of = (my_ctx if half == 0 else 2 * CTX - 1 - my_ctx) * PIECE + lax.broadcasted_iota(jnp.int32, (PIECE, width), 0)
        key = lax.broadcasted_iota(jnp.int32, (PIECE, width), 1)
        up_piece = 2 * CTX - 1 - (key - low_keys) // PIECE
        k_rank_of = jnp.where(key < low_keys, key, up_piece * PIECE + lax.rem(key, PIECE))
        start = 0 if half == 0 else low_keys
        cap[:, start:start + width] = jnp.where(k_rank_of <= q_rank_of, POS_BIG, NEG_BIG)

    x_copy.wait()
    kr_copy.wait()
    rot = jnp.dot(x_ref[...], wkr_ref[...], preferred_element_type=jnp.float32)
    rot = jnp.concatenate([rot, rot], axis=1)
    k_rot = rotate(rot, cos_ref[:, :2 * ROPE], sin_ref[:, :2 * ROPE]).astype(jnp.bfloat16)
    dkv_copy.wait()
    c_kv = rms_norm(jnp.dot(x_ref[...], wdown[0], preferred_element_type=jnp.float32), gkv_ref[...]).astype(jnp.bfloat16)
    for half in range(2):
        rows = slice(half * PIECE, (half + 1) * PIECE)
        lat[half, my_ctx, :, :lat_rank] = c_kv[rows]
        lat[half, my_ctx, :, lat_rank:] = k_rot[rows]

    @pl.when((my_tp > 0) & (my_tp < TP - 1))
    def _():
        pl.semaphore_wait(barrier, 4)

    @pl.when((my_tp == 0) | (my_tp == TP - 1))
    def _():
        pl.semaphore_wait(barrier, 3)

    def lat_copy(owner, peer, sem):
        part = lat.at[:, owner]
        return pltpu.make_async_remote_copy(src_ref=part, dst_ref=part, send_sem=lat_send.at[sem], recv_sem=lat_recv.at[sem],
                                            device_id={'ctx': peer}, device_id_type=MESH_ID)

    lat_copy(my_ctx, across, 1).start()
    lat_copy(my_ctx, partner, 0).start()

    def dq_step(blk, _):
        @pl.when(blk + 1 < n_down)
        def _():
            dq_copy(blk + 1).start()

        @pl.when(blk + 1 == n_down)
        def _():
            start_all(q_copies(0))
            start_all(q_copies(1))

        dq_copy(blk).wait()
        cols = pl.ds(pl.multiple_of((blk - 1) * DOWN_BLK, DOWN_BLK), DOWN_BLK)
        cq_f[:, cols] = jnp.dot(x_ref[...], wdown[lax.rem(blk, 2)], preferred_element_type=jnp.float32)
        return 0

    lax.fori_loop(1, n_down, dq_step, 0)
    cq[...] = rms_norm(cq_f[...], gq_ref[...]).astype(jnp.bfloat16)

    def q_step(grp, _):
        slot = lax.rem(grp, 2)
        wait_all(q_copies(grp))
        qn[grp] = jnp.dot(cq[...], wq[slot], preferred_element_type=jnp.float32).astype(jnp.bfloat16)
        q_rot = jnp.dot(cq[...], wqr[slot], preferred_element_type=jnp.float32)
        qp[grp] = rotate(q_rot, cos_ref[...], sin_ref[...]).astype(jnp.bfloat16)

        @pl.when(grp + 2 < groups)
        def _():
            start_all(q_copies(grp + 2))

        @pl.when(grp + 2 == groups)
        def _():
            start_all(kv_copies(0))
            start_all(kv_copies(1))

        @pl.when(grp == RELAY_AT)
        def _():
            lat_copy(across, across, 1).wait_recv()
            lat_copy(across, partner, 2).start()
        return 0

    lax.fori_loop(0, groups, q_step, 0)
    for step in range(O_SLOTS - 1):
        start_all(o_copies(step))
    lat_copy(partner, partner, 0).wait_recv()
    lat_copy(across, partner, 2).wait_recv()

    lane = lax.broadcasted_iota(jnp.int32, (n_keys, 2 * ROPE), 1)
    both = lat[:, :, :, lat_rank:].reshape(n_keys, 2 * ROPE)
    zero = jnp.zeros_like(both)
    kpe[0] = jnp.where(lane < ROPE, both, zero)
    kpe[1] = jnp.where(lane < ROPE, zero, both)

    expo_scale = (NOPE + ROPE) ** -0.5 * math.log2(math.e)
    nt = (((1,), (1,)), ((), ()))

    def attend(scores, caps, values):
        scores = jnp.minimum(scores, caps)
        top = jnp.max(scores, axis=-1, keepdims=True)
        prob = jnp.exp2((scores - top) * expo_scale)
        total = jnp.sum(prob, axis=-1, keepdims=True)
        out = jnp.dot(prob.astype(jnp.bfloat16), values, preferred_element_type=jnp.float32)
        return (out / total).astype(jnp.bfloat16)

    def head_step(grp, _):
        slot = lax.rem(grp, 2)
        wait_all(kv_copies(grp))
        c_all = lat[:, :, :, :lat_rank].reshape(n_keys, lat_rank)
        k_all = jnp.dot(c_all, wkv[slot, 0], preferred_element_type=jnp.float32).astype(jnp.bfloat16)
        v_all = jnp.dot(c_all, wkv[slot, 1], preferred_element_type=jnp.float32).astype(jnp.bfloat16)

        @pl.when(grp + 2 < groups)
        def _():
            start_all(kv_copies(grp + 2))

        for head in range(GROUP):
            cols = slice(head * NOPE, (head + 1) * NOPE)
            pair = slice((head // 2) * 2 * ROPE, (head // 2 + 1) * 2 * ROPE)
            q_cat = jnp.concatenate([qn[grp, :, cols], qp[grp, :, pair]], axis=1)
            k_cat = jnp.concatenate([k_all[:, cols], kpe[head % 2]], axis=1)
            v_head = v_all[:, cols]
            s_low = lax.dot_general(q_cat, k_cat[:low_keys], nt, preferred_element_type=jnp.float32)
            s_up = lax.dot_general(q_cat[PIECE:], k_cat[low_keys:], nt, preferred_element_type=jnp.float32)
            out_cols = pl.ds(pl.multiple_of(grp * (GROUP * VALUE), GROUP * VALUE) + head * VALUE, VALUE)
            o_ref[:PIECE, out_cols] = attend(s_low[:PIECE], cap[:, :low_keys], v_head[:low_keys])
            s_both = jnp.concatenate([s_low[PIECE:], s_up], axis=1)
            o_ref[PIECE:, out_cols] = attend(s_both, cap[:, low_keys:], v_head)
        return 0

    lax.fori_loop(0, groups, head_step, 0)

    depth = (TP - 1 - my_tp, my_tp)
    onward = (left, right)
    back = (right, left)

    def y_slice(side, chunk):
        step, row = chunk // row_blks, lax.rem(chunk, row_blks)
        return (pl.ds(pl.multiple_of(row * PIECE, PIECE), PIECE),
                pl.ds(pl.multiple_of(side * half_cols + step * COL_BLK, COL_BLK), COL_BLK))

    def f_copy(side, chunk):
        return pltpu.make_async_remote_copy(
            src_ref=acc.at[side, chunk], dst_ref=rbuf.at[side, chunk],
            send_sem=f_send.at[side, chunk], recv_sem=f_recv.at[side, chunk],
            device_id={'tp': onward[side]}, device_id_type=MESH_ID)

    def b_copy(side, chunk):
        part = y_ref.at[y_slice(side, chunk)]
        return pltpu.make_async_remote_copy(
            src_ref=part, dst_ref=part,
            send_sem=b_send.at[side, chunk], recv_sem=b_recv.at[side, chunk],
            device_id={'tp': back[side]}, device_id_type=MESH_ID)

    def reduce_event(side, event):
        chunk = event - SUM_LAG * (depth[side] - 1)
        live = (chunk >= 0) & (chunk < n_chunks)

        @pl.when(live & (depth[side] > 0))
        def _():
            f_copy(side, chunk).wait_recv()

        @pl.when(live & (depth[side] > 0) & (depth[side] < TP - 1))
        def _():
            acc[side, chunk] = acc[side, chunk] + rbuf[side, chunk]
            f_copy(side, chunk).start()

        @pl.when(live & (depth[side] == TP - 1))
        def _():
            total = acc[side, chunk] + rbuf[side, chunk]
            y_ref[y_slice(side, chunk)] = total.astype(y_ref.dtype)
            b_copy(side, chunk).start()

    def out_step(step, _):
        slot = lax.rem(step, O_SLOTS)

        @pl.when(step + O_SLOTS - 1 < col_steps)
        def _():
            start_all(o_copies(step + O_SLOTS - 1))

        wait_all(o_copies(step))
        part = jnp.dot(o_ref[...], wo[slot], preferred_element_type=jnp.float32)
        for side in range(2):
            for row in range(row_blks):
                chunk = step * row_blks + row
                acc[side, chunk] = part[row * PIECE:(row + 1) * PIECE, side * COL_BLK:(side + 1) * COL_BLK]

                @pl.when(depth[side] == 0)
                def _():
                    f_copy(side, chunk).start()

        @pl.when(step >= FIRST_EVENT)
        def _():
            for side in range(2):
                reduce_event(side, step - FIRST_EVENT)
        return 0

    lax.fori_loop(0, col_steps, out_step, 0)

    def late_event(event, _):
        for side in range(2):
            reduce_event(side, event)
        return 0

    lax.fori_loop(col_steps - FIRST_EVENT, n_chunks + SUM_LAG * (TP - 2), late_event, 0)

    def back_event(event, _):
        for side in range(2):
            chunk = event - BACK_LAG * (TP - 2 - depth[side])
            live = (chunk >= 0) & (chunk < n_chunks)

            @pl.when(live & (depth[side] < TP - 1))
            def _():
                b_copy(side, chunk).wait_recv()

            @pl.when(live & (depth[side] > 0) & (depth[side] < TP - 1))
            def _():
                b_copy(side, chunk).start()
        return 0

    lax.fori_loop(0, n_chunks + BACK_LAG * (TP - 2), back_event, 0)

    lat_copy(my_ctx, partner, 0).wait_send()
    lat_copy(my_ctx, across, 1).wait_send()
    lat_copy(across, partner, 2).wait_send()

    def drain(chunk, _):
        for side in range(2):
            @pl.when(depth[side] < TP - 1)
            def _():
                f_copy(side, chunk).wait_send()

            @pl.when(depth[side] > 0)
            def _():
                b_copy(side, chunk).wait_send()
        return 0

    lax.fori_loop(0, n_chunks, drain, 0)


def layer(tok_x, tok_pos, w_dq, g_q, w_uq, w_qr, w_dkv, g_kv, w_kr, w_uk, w_uv, w_o):
    n_rows, model_dim = tok_x.shape
    q_rank, lat_rank = w_dq.shape[1], w_dkv.shape[1]
    heads = w_uq.shape[1] // NOPE
    groups = heads // GROUP
    n_keys = CTX * n_rows
    n_chunks = (model_dim // 2 // COL_BLK) * (n_rows // PIECE)
    bf16, f32 = jnp.bfloat16, jnp.float32
    cos_t, sin_t = rope_tables(tok_pos, GROUP)
    vmem = pl.BlockSpec(memory_space=pltpu.VMEM)
    hbm = pl.BlockSpec(memory_space=pl.ANY)
    dma = pltpu.SemaphoreType.DMA
    return pl.pallas_call(
        layer_kernel,
        out_shape=jax.ShapeDtypeStruct((n_rows, model_dim), bf16),
        in_specs=[hbm, vmem, vmem, vmem, vmem] + [hbm] * 8,
        out_specs=vmem,
        scratch_shapes=[
            pltpu.VMEM((n_rows, model_dim), bf16),
            pltpu.VMEM((model_dim, ROPE), bf16),
            pltpu.VMEM((2, model_dim, DOWN_BLK), bf16),
            pltpu.VMEM((2, q_rank, GROUP * NOPE), bf16),
            pltpu.VMEM((2, q_rank, GROUP * ROPE), bf16),
            pltpu.VMEM((2, 2, lat_rank, GROUP * NOPE), bf16),
            pltpu.VMEM((O_SLOTS, heads * VALUE, 2 * COL_BLK), bf16),
            pltpu.VMEM((2, CTX, PIECE, lat_rank + 2 * ROPE), bf16),
            pltpu.VMEM((2, n_keys, 2 * ROPE), bf16),
            pltpu.VMEM((n_rows, q_rank), f32),
            pltpu.VMEM((n_rows, q_rank), bf16),
            pltpu.VMEM((groups, n_rows, GROUP * NOPE), bf16),
            pltpu.VMEM((groups, n_rows, GROUP * ROPE), bf16),
            pltpu.VMEM((PIECE, n_keys // 2 + n_keys), f32),
            pltpu.VMEM((n_rows, heads * VALUE), bf16),
            pltpu.VMEM((2, n_chunks, PIECE, COL_BLK), f32),
            pltpu.VMEM((2, n_chunks, PIECE, COL_BLK), f32),
            dma, dma, dma((2,)), dma((2, 2)), dma((2, 2)), dma((O_SLOTS, 2)),
            dma((3,)), dma((3,)),
            dma((2, n_chunks)), dma((2, n_chunks)), dma((2, n_chunks)), dma((2, n_chunks)),
        ],
        compiler_params=pltpu.CompilerParams(collective_id=0, has_side_effects=True, vmem_limit_bytes=67043328),
        name='layer',
    )(tok_x, cos_t, sin_t, g_q.astype(f32)[None], g_kv.astype(f32)[None], w_dq, w_uq, w_qr, w_dkv, w_kr, w_uk, w_uv, w_o)


def solution(mesh):
    tok_spec = P(('dp', 'ctx'), None)
    pos_spec = P(('dp', 'ctx'))
    full_mat = P(None, None)
    full_vec = P(None)
    col_spec = P(None, 'tp')
    row_spec = P('tp', None)
    return jax.shard_map(layer, mesh=mesh,
                         in_specs=(tok_spec, pos_spec, full_mat, full_vec, col_spec, col_spec, full_mat, full_vec, full_mat, col_spec, col_spec, row_spec),
                         out_specs=tok_spec, check_vma=False)
```

```python
import math

import jax
import jax.numpy as jnp
import numpy as np
from jax import lax
from jax.experimental import pallas as pl
from jax.experimental.pallas import tpu as pltpu
from jax.sharding import PartitionSpec as P

ROPE_BASE = 10000.0
NORM_EPS = 1e-6
NEG_BIG = -1e30
POS_BIG = 3e38
TP = 4
CTX = 4
PIECE = 128
NOPE = 128
ROPE = 64
VALUE = 128
GROUP = 4
DOWN_BLK = 512
COL_BLK = 256
O_SLOTS = 3
LOW_FIRST = 4
HIGH_FIRST = 5
EVENTS_OUT = 3
SUM_LAG = 2
BACK_LAG = 3
MESH_ID = pl.DeviceIdType.MESH


def inv_freq_row():
    half_dim = ROPE // 2
    inv_freq = np.float32(ROPE_BASE) ** (-np.arange(half_dim, dtype=np.float32) * np.float32(2.0) / np.float32(ROPE))
    return np.tile(inv_freq.astype(np.float32), 4)[None]


def rms_norm(act_in, gain_row):
    inv_rms = lax.rsqrt(jnp.mean(act_in * act_in, axis=-1, keepdims=True) + NORM_EPS)
    return act_in * inv_rms * gain_row


def rotate(rows, cos_t, sin_t):
    width = rows.shape[1]
    lane = lax.broadcasted_iota(jnp.int32, rows.shape, 1)
    swapped = jnp.where(lax.rem(lane, ROPE) < ROPE // 2,
                        pltpu.roll(rows, width - ROPE // 2, 1), pltpu.roll(rows, ROPE // 2, 1))
    return rows * cos_t + swapped * sin_t


def layer_kernel(x_hbm, pos_ref, freq_ref, gq_ref, gkv_ref, wdq_hbm, wuq_hbm, wqr_hbm, wdkv_hbm, wkr_hbm, wuk_hbm, wuv_hbm, wo_hbm,
                 y_ref,
                 x_ref, wkr_ref, wbig, wq, wqr, wkv,
                 cos_ref, sin_ref, lat, kpe, cq_f, cq, qn, qp, kv_low, cap, o_ref, acc, rbuf,
                 x_sem, kr_sem, down_sem, q_sem, kv_sem, o_sem,
                 lat_send, lat_recv, f_send, f_recv, b_send, b_recv):
    my_tp = lax.axis_index('tp')
    my_ctx = lax.axis_index('ctx')
    n_rows, n_cols = y_ref.shape
    heads = o_ref.shape[1] // VALUE
    groups = heads // GROUP
    q_rank = cq.shape[1]
    lat_rank = wkv.shape[2]
    n_keys = 2 * CTX * PIECE
    low_keys = CTX * PIECE
    n_down = 1 + q_rank // DOWN_BLK
    left = lax.rem(my_tp + TP - 1, TP)
    right = lax.rem(my_tp + 1, TP)
    partner = my_ctx + 1 - 2 * lax.rem(my_ctx, 2)
    across = lax.rem(my_ctx + 2, CTX)

    x_copy = pltpu.make_async_copy(x_hbm, x_ref, x_sem)
    kr_copy = pltpu.make_async_copy(wkr_hbm, wkr_ref, kr_sem)

    def dq_copy(blk):
        cols = pl.ds(pl.multiple_of((blk - 1) * DOWN_BLK, DOWN_BLK), DOWN_BLK)
        slot = lax.rem(blk, 2)
        return pltpu.make_async_copy(wdq_hbm.at[:, cols], wbig.at[slot], down_sem.at[slot])

    dkv_copy = pltpu.make_async_copy(wdkv_hbm, wbig.at[0], down_sem.at[0])

    def q_copies(grp):
        slot = lax.rem(grp, 2)
        n_blk, r_blk = GROUP * NOPE, GROUP * ROPE
        return (pltpu.make_async_copy(wuq_hbm.at[:, pl.ds(pl.multiple_of(grp * n_blk, n_blk), n_blk)], wq.at[slot], q_sem.at[slot, 0]),
                pltpu.make_async_copy(wqr_hbm.at[:, pl.ds(pl.multiple_of(grp * r_blk, r_blk), r_blk)], wqr.at[slot], q_sem.at[slot, 1]))

    def kv_copies(turn):
        grp, slot = lax.rem(turn, groups), lax.rem(turn, 2)
        n_blk = GROUP * NOPE
        cols = pl.ds(pl.multiple_of(grp * n_blk, n_blk), n_blk)
        return (pltpu.make_async_copy(wuk_hbm.at[:, cols], wkv.at[slot, 0], kv_sem.at[slot, 0]),
                pltpu.make_async_copy(wuv_hbm.at[:, cols], wkv.at[slot, 1], kv_sem.at[slot, 1]))

    row_blks = n_rows // PIECE
    half_cols = n_cols // 2
    col_steps = half_cols // COL_BLK
    n_chunks = col_steps * row_blks

    def o_copies(turn):
        step, slot = lax.rem(turn, col_steps), lax.rem(turn, O_SLOTS)
        return [pltpu.make_async_copy(
            wo_hbm.at[:, pl.ds(pl.multiple_of(side * half_cols + step * COL_BLK, COL_BLK), COL_BLK)],
            wbig.at[slot, pl.ds(0, heads * VALUE), pl.ds(side * COL_BLK, COL_BLK)], o_sem.at[slot, side]) for side in range(2)]

    def start_all(copies):
        for copy in copies:
            copy.start()

    def wait_all(copies):
        for copy in copies:
            copy.wait()

    x_copy.start()
    kr_copy.start()
    dkv_copy.start()
    dq_copy(1).start()

    barrier = pltpu.get_barrier_semaphore()
    for peer in (partner, across):
        pl.semaphore_signal(barrier, inc=1, device_id={'ctx': peer}, device_id_type=MESH_ID)

    @pl.when(my_tp > 0)
    def _():
        pl.semaphore_signal(barrier, inc=1, device_id={'tp': left}, device_id_type=MESH_ID)

    @pl.when(my_tp < TP - 1)
    def _():
        pl.semaphore_signal(barrier, inc=1, device_id={'tp': right}, device_id_type=MESH_ID)

    row = lax.broadcasted_iota(jnp.int32, (n_rows, n_rows), 0)
    col = lax.broadcasted_iota(jnp.int32, (n_rows, n_rows), 1)
    pos_row = pos_ref[...].astype(jnp.float32).reshape(1, n_rows)
    pos_col = jnp.sum(jnp.where(row == col, pos_row, 0.0), axis=1, keepdims=True)
    angles = pos_col * freq_ref[...]
    lane_of = lax.broadcasted_iota(jnp.int32, angles.shape, 1)
    cos_t = jnp.cos(angles)
    sin_t = jnp.where(lax.rem(lane_of, ROPE) < ROPE // 2, -1.0, 1.0) * jnp.sin(angles)
    for copy in range(GROUP // 2):
        cos_ref[:, copy * 2 * ROPE:(copy + 1) * 2 * ROPE] = cos_t
        sin_ref[:, copy * 2 * ROPE:(copy + 1) * 2 * ROPE] = sin_t

    for half, width in ((0, low_keys), (1, n_keys)):
        q_rank_of = (my_ctx if half == 0 else 2 * CTX - 1 - my_ctx) * PIECE + lax.broadcasted_iota(jnp.int32, (PIECE, width), 0)
        key = lax.broadcasted_iota(jnp.int32, (PIECE, width), 1)
        up_piece = 2 * CTX - 1 - (key - low_keys) // PIECE
        k_rank_of = jnp.where(key < low_keys, key, up_piece * PIECE + lax.rem(key, PIECE))
        start = 0 if half == 0 else low_keys
        cap[:, start:start + width] = jnp.where(k_rank_of <= q_rank_of, POS_BIG, NEG_BIG)

    x_copy.wait()
    kr_copy.wait()
    rot = lax.dot_general(x_ref[...], wkr_ref[...], (((1,), (1,)), ((), ())), preferred_element_type=jnp.float32)
    rot = jnp.concatenate([rot, rot], axis=1)
    k_rot = rotate(rot, cos_ref[:, :2 * ROPE], sin_ref[:, :2 * ROPE]).astype(jnp.bfloat16)
    dkv_copy.wait()
    c_kv = rms_norm(jnp.dot(x_ref[...], wbig[0], preferred_element_type=jnp.float32), gkv_ref[...].astype(jnp.float32).reshape(1, lat_rank)).astype(jnp.bfloat16)
    for half in range(2):
        rows = slice(half * PIECE, (half + 1) * PIECE)
        lat[half, my_ctx, :, :lat_rank] = c_kv[rows]
        lat[half, my_ctx, :, lat_rank:] = k_rot[rows]

    @pl.when((my_tp > 0) & (my_tp < TP - 1))
    def _():
        pl.semaphore_wait(barrier, 4)

    @pl.when((my_tp == 0) | (my_tp == TP - 1))
    def _():
        pl.semaphore_wait(barrier, 3)

    def lat_copy(owner, peer, sem):
        part = lat.at[:, owner]
        return pltpu.make_async_remote_copy(src_ref=part, dst_ref=part, send_sem=lat_send.at[sem], recv_sem=lat_recv.at[sem],
                                            device_id={'ctx': peer}, device_id_type=MESH_ID)

    lat_copy(my_ctx, across, 1).start()
    lat_copy(my_ctx, partner, 0).start()

    def dq_step(blk, _):
        @pl.when(blk + 1 < n_down)
        def _():
            dq_copy(blk + 1).start()

        @pl.when(blk + 1 == n_down)
        def _():
            for grp in range(2):
                start_all(q_copies(grp))
                start_all(kv_copies(grp))

        dq_copy(blk).wait()
        cols = pl.ds(pl.multiple_of((blk - 1) * DOWN_BLK, DOWN_BLK), DOWN_BLK)
        cq_f[:, cols] = jnp.dot(x_ref[...], wbig[lax.rem(blk, 2)], preferred_element_type=jnp.float32)
        return 0

    lax.fori_loop(1, n_down, dq_step, 0)
    cq[...] = rms_norm(cq_f[...], gq_ref[...].astype(jnp.float32).reshape(1, q_rank)).astype(jnp.bfloat16)

    for turn in range(O_SLOTS - 1):
        start_all(o_copies(turn))

    lat_copy(across, across, 1).wait_recv()
    lat_copy(across, partner, 2).start()
    lat_copy(partner, partner, 0).wait_recv()
    lat_copy(across, partner, 2).wait_recv()

    lane = lax.broadcasted_iota(jnp.int32, (n_keys, 2 * ROPE), 1)
    k_rots = lat[:, :, :, lat_rank:].reshape(n_keys, 2 * ROPE)
    zero = jnp.zeros_like(k_rots)
    kpe[0] = jnp.where(lane < ROPE, k_rots, zero)
    kpe[1] = jnp.where(lane < ROPE, zero, k_rots)

    expo_scale = (NOPE + ROPE) ** -0.5 * math.log2(math.e)

    def attend(q_nope, q_rot, keys, k_rots, values, caps):
        k_cat = jnp.concatenate([keys, k_rots], axis=1)
        q_cat = jnp.concatenate([q_nope, q_rot], axis=1)
        scores = lax.dot_general(q_cat, k_cat, (((1,), (1,)), ((), ())), preferred_element_type=jnp.float32)
        scores = jnp.minimum(scores, caps)
        top = jnp.max(scores, axis=-1, keepdims=True)
        prob = jnp.exp2((scores - top) * expo_scale)
        total = jnp.sum(prob, axis=-1, keepdims=True)
        out = jnp.dot(prob.astype(jnp.bfloat16), values, preferred_element_type=jnp.float32)
        return (out / total).astype(jnp.bfloat16)

    def up_project(half, slot):
        rows = lat[half, :, :, :lat_rank].reshape(low_keys, lat_rank)
        return [jnp.dot(rows, wkv[slot, part], preferred_element_type=jnp.float32).astype(jnp.bfloat16) for part in range(2)]

    def out_cols(grp, head):
        return pl.ds(pl.multiple_of(grp * (GROUP * VALUE), GROUP * VALUE) + head * VALUE, VALUE)

    def low_step(grp, _):
        slot = lax.rem(grp, 2)
        wait_all(q_copies(grp))
        wait_all(kv_copies(grp))
        q_nope = jnp.dot(cq[...], wq[slot], preferred_element_type=jnp.float32).astype(jnp.bfloat16)
        q_rot = jnp.dot(cq[...], wqr[slot], preferred_element_type=jnp.float32)
        q_rot = rotate(q_rot, cos_ref[...], sin_ref[...]).astype(jnp.bfloat16)
        qn[grp] = q_nope[PIECE:]
        qp[grp] = q_rot[PIECE:]
        k_low, v_low = up_project(0, slot)
        kv_low[grp, 0] = k_low
        kv_low[grp, 1] = v_low
        for head in range(GROUP):
            cols = slice(head * NOPE, (head + 1) * NOPE)
            pair = slice((head // 2) * 2 * ROPE, (head // 2 + 1) * 2 * ROPE)
            o_ref[:PIECE, out_cols(grp, head)] = attend(
                q_nope[:PIECE, cols], q_rot[:PIECE, pair], k_low[:, cols], kpe[head % 2, :low_keys], v_low[:, cols], cap[:, :low_keys])

        start_all(kv_copies(grp + 2))

        @pl.when(grp + 2 < groups)
        def _():
            start_all(q_copies(grp + 2))
        return 0

    lax.fori_loop(0, groups, low_step, 0)

    def high_step(grp):
        slot = lax.rem(grp, 2)
        wait_all(kv_copies(groups + grp))
        k_up, v_up = up_project(1, slot)
        for head in range(GROUP):
            cols = slice(head * NOPE, (head + 1) * NOPE)
            pair = slice((head // 2) * 2 * ROPE, (head // 2 + 1) * 2 * ROPE)
            keys = jnp.concatenate([kv_low[grp, 0, :, cols], k_up[:, cols]], axis=0)
            values = jnp.concatenate([kv_low[grp, 1, :, cols], v_up[:, cols]], axis=0)
            o_ref[PIECE:, out_cols(grp, head)] = attend(
                qn[grp, :, cols], qp[grp, :, pair], keys, kpe[head % 2], values, cap[:, low_keys:])

        @pl.when(grp + 2 < groups)
        def _():
            start_all(kv_copies(groups + grp + 2))

    depth = (TP - 1 - my_tp, my_tp)
    onward = (left, right)
    back = (right, left)

    def y_slice(side, chunk):
        row, step = chunk // col_steps, lax.rem(chunk, col_steps)
        return (pl.ds(pl.multiple_of(row * PIECE, PIECE), PIECE),
                pl.ds(pl.multiple_of(side * half_cols + step * COL_BLK, COL_BLK), COL_BLK))

    def f_copy(side, chunk):
        return pltpu.make_async_remote_copy(
            src_ref=acc.at[side, chunk], dst_ref=rbuf.at[side, chunk],
            send_sem=f_send.at[side, chunk], recv_sem=f_recv.at[side, chunk],
            device_id={'tp': onward[side]}, device_id_type=MESH_ID)

    def b_copy(side, chunk):
        part = y_ref.at[y_slice(side, chunk)]
        return pltpu.make_async_remote_copy(
            src_ref=part, dst_ref=part,
            send_sem=b_send.at[side, chunk], recv_sem=b_recv.at[side, chunk],
            device_id={'tp': back[side]}, device_id_type=MESH_ID)

    def reduce_event(side, event, row):
        chunk = event - SUM_LAG * (depth[side] - 1)
        live = (chunk >= 0) & (chunk < col_steps)
        chunk = chunk + row * col_steps

        @pl.when(live & (depth[side] > 0))
        def _():
            f_copy(side, chunk).wait_recv()

        @pl.when(live & (depth[side] > 0) & (depth[side] < TP - 1))
        def _():
            acc[side, chunk] = acc[side, chunk] + rbuf[side, chunk]
            f_copy(side, chunk).start()

        @pl.when(live & (depth[side] == TP - 1))
        def _():
            total = acc[side, chunk] + rbuf[side, chunk]
            y_ref[y_slice(side, chunk)] = total.astype(y_ref.dtype)
            b_copy(side, chunk).start()

    def back_event(side, event, row):
        chunk = event - BACK_LAG * (TP - 2 - depth[side])
        live = (chunk >= 0) & (chunk < col_steps)
        chunk = chunk + row * col_steps

        @pl.when(live & (depth[side] < TP - 1))
        def _():
            b_copy(side, chunk).wait_recv()

        @pl.when(live & (depth[side] > 0) & (depth[side] < TP - 1))
        def _():
            b_copy(side, chunk).start()

    def both(event_fn, event, row):
        for side in range(2):
            event_fn(side, event, row)

    def project(row, step):
        turn = row * col_steps + step

        @pl.when(turn + O_SLOTS - 1 < row_blks * col_steps)
        def _():
            start_all(o_copies(turn + O_SLOTS - 1))

        wait_all(o_copies(turn))
        part = jnp.dot(o_ref[row * PIECE:(row + 1) * PIECE], wbig[lax.rem(turn, O_SLOTS), :heads * VALUE], preferred_element_type=jnp.float32)
        for side in range(2):
            acc[side, turn] = part[:, side * COL_BLK:(side + 1) * COL_BLK]

            @pl.when(depth[side] == 0)
            def _():
                f_copy(side, turn).start()

    sum_events = col_steps + SUM_LAG * (TP - 2)
    back_events = col_steps + BACK_LAG * (TP - 2)

    def low_out(step, _):
        project(0, step)

        @pl.when((step >= LOW_FIRST) & (lax.rem(step, 2) == 0))
        def _():
            both(reduce_event, (step - LOW_FIRST) // 2, 0)
        return 0

    lax.fori_loop(0, col_steps, low_out, 0)

    def high_attention(grp, _):
        high_step(grp)

        @pl.when(lax.rem(grp, 4) != 3)
        def _():
            both(reduce_event, EVENTS_OUT + grp - grp // 4, 0)
        return 0

    lax.fori_loop(0, groups, high_attention, 0)

    first_sum = EVENTS_OUT + groups - groups // 4

    def high_out(step, _):
        project(1, step)

        @pl.when((lax.rem(step, 2) == 0) & (first_sum + step // 2 < sum_events))
        def _():
            both(reduce_event, first_sum + step // 2, 0)

        @pl.when(step >= HIGH_FIRST)
        def _():
            both(back_event, step - HIGH_FIRST, 0)
        return 0

    lax.fori_loop(0, col_steps, high_out, 0)

    first_back = col_steps - HIGH_FIRST
    for event in range(first_sum + (col_steps + 1) // 2, sum_events):
        both(reduce_event, event, 0)

    def high_sum(event, _):
        both(reduce_event, event, 1)

        @pl.when(first_back + event < back_events)
        def _():
            both(back_event, first_back + event, 0)
        return 0

    lax.fori_loop(0, sum_events, high_sum, 0)
    for event in range(first_back + sum_events, back_events):
        both(back_event, event, 0)

    def high_back(event, _):
        both(back_event, event, 1)
        return 0

    lax.fori_loop(0, back_events, high_back, 0)

    lat_copy(my_ctx, partner, 0).wait_send()
    lat_copy(my_ctx, across, 1).wait_send()
    lat_copy(across, partner, 2).wait_send()

    def drain(chunk, _):
        for side in range(2):
            @pl.when(depth[side] < TP - 1)
            def _():
                f_copy(side, chunk).wait_send()

            @pl.when(depth[side] > 0)
            def _():
                b_copy(side, chunk).wait_send()
        return 0

    lax.fori_loop(0, n_chunks, drain, 0)


def layer(tok_x, tok_pos, w_dq, g_q, w_uq, w_qr, w_dkv, g_kv, w_kr, w_uk, w_uv, w_o):
    n_rows, model_dim = tok_x.shape
    q_rank, lat_rank = w_dq.shape[1], w_dkv.shape[1]
    heads = w_uq.shape[1] // NOPE
    groups = heads // GROUP
    n_keys = CTX * n_rows
    n_chunks = (model_dim // 2 // COL_BLK) * (n_rows // PIECE)
    bf16, f32 = jnp.bfloat16, jnp.float32
    vmem = pl.BlockSpec(memory_space=pltpu.VMEM)
    hbm = pl.BlockSpec(memory_space=pl.ANY)
    dma = pltpu.SemaphoreType.DMA
    return pl.pallas_call(
        layer_kernel,
        out_shape=jax.ShapeDtypeStruct((n_rows, model_dim), bf16),
        in_specs=[hbm, vmem, vmem, vmem, vmem] + [hbm] * 8,
        out_specs=vmem,
        scratch_shapes=[
            pltpu.VMEM((n_rows, model_dim), bf16),
            pltpu.VMEM((ROPE, model_dim), bf16),
            pltpu.VMEM((O_SLOTS, model_dim, DOWN_BLK), bf16),
            pltpu.VMEM((2, q_rank, GROUP * NOPE), bf16),
            pltpu.VMEM((2, q_rank, GROUP * ROPE), bf16),
            pltpu.VMEM((2, 2, lat_rank, GROUP * NOPE), bf16),
            pltpu.VMEM((n_rows, GROUP * ROPE), f32),
            pltpu.VMEM((n_rows, GROUP * ROPE), f32),
            pltpu.VMEM((2, CTX, PIECE, lat_rank + 2 * ROPE), bf16),
            pltpu.VMEM((2, n_keys, 2 * ROPE), bf16),
            pltpu.VMEM((n_rows, q_rank), f32),
            pltpu.VMEM((n_rows, q_rank), bf16),
            pltpu.VMEM((groups, PIECE, GROUP * NOPE), bf16),
            pltpu.VMEM((groups, PIECE, GROUP * ROPE), bf16),
            pltpu.VMEM((groups, 2, n_keys // 2, GROUP * NOPE), bf16),
            pltpu.VMEM((PIECE, n_keys // 2 + n_keys), f32),
            pltpu.VMEM((n_rows, heads * VALUE), bf16),
            pltpu.VMEM((2, n_chunks, PIECE, COL_BLK), f32),
            pltpu.VMEM((2, n_chunks, PIECE, COL_BLK), f32),
            dma, dma, dma((2,)), dma((2, 2)), dma((2, 2)), dma((O_SLOTS, 2)),
            dma((3,)), dma((3,)),
            dma((2, n_chunks)), dma((2, n_chunks)), dma((2, n_chunks)), dma((2, n_chunks)),
        ],
        compiler_params=pltpu.CompilerParams(collective_id=0, has_side_effects=True, vmem_limit_bytes=67043328),
        name='layer',
    )(tok_x, tok_pos, jnp.asarray(inv_freq_row()), g_q, g_kv, w_dq, w_uq, w_qr, w_dkv, w_kr.T, w_uk, w_uv, w_o)


def solution(mesh):
    tok_spec = P(('dp', 'ctx'), None)
    pos_spec = P(('dp', 'ctx'))
    full_mat = P(None, None)
    full_vec = P(None)
    col_spec = P(None, 'tp')
    row_spec = P('tp', None)
    return jax.shard_map(layer, mesh=mesh,
                         in_specs=(tok_spec, pos_spec, full_mat, full_vec, col_spec, col_spec, full_mat, full_vec, full_mat, col_spec, col_spec, row_spec),
                         out_specs=tok_spec, check_vma=False)
```

```python
import math

import jax
import jax.numpy as jnp
import numpy as np
from jax import lax
from jax.experimental import pallas as pl
from jax.experimental.pallas import tpu as pltpu
from jax.sharding import PartitionSpec as P

ROPE_BASE = 10000.0
NORM_EPS = 1e-6
NEG_BIG = -1e30
POS_BIG = 3e38
TP = 4
CTX = 4
PIECE = 128
NOPE = 128
ROPE = 64
VALUE = 128
GROUP = 4
DOWN_BLK = 512
COL_BLK = 256
O_SLOTS = 3
LOW_FIRST = 4
HIGH_FIRST = 5
EVENTS_OUT = 3
RELAY_AT = 5
EXTRA = 2
LOW_WIDE = 4
HIGH_WIDE = 2
SUM_LAG = 2
BACK_LAG = (2, 3)
MESH_ID = pl.DeviceIdType.MESH


def inv_freq_row():
    half_dim = ROPE // 2
    inv_freq = np.float32(ROPE_BASE) ** (-np.arange(half_dim, dtype=np.float32) * np.float32(2.0) / np.float32(ROPE))
    return np.tile(inv_freq.astype(np.float32), 4)[None]


def rms_norm(act_in, gain_row):
    inv_rms = lax.rsqrt(jnp.mean(act_in * act_in, axis=-1, keepdims=True) + NORM_EPS)
    return act_in * inv_rms * gain_row


def rotate(rows, cos_t, sin_t):
    width = rows.shape[1]
    lane = lax.broadcasted_iota(jnp.int32, rows.shape, 1)
    swapped = jnp.where(lax.rem(lane, ROPE) < ROPE // 2,
                        pltpu.roll(rows, width - ROPE // 2, 1), pltpu.roll(rows, ROPE // 2, 1))
    return rows * cos_t + swapped * sin_t


def layer_kernel(x_hbm, pos_ref, freq_ref, gq_ref, gkv_ref, wdq_hbm, wuq_hbm, wqr_hbm, wdkv_hbm, wkr_hbm, wuk_hbm, wuv_hbm, wo_hbm,
                 y_hbm,
                 y_ref, x_ref, wkr_ref, wbig, wq, wqr, wkv,
                 cos_ref, sin_ref, lat, kpe, cq_f, cq, qn, qp, kv_low, cap, o_ref, acc, rbuf,
                 x_sem, kr_sem, down_sem, q_sem, kv_sem, o_sem,
                 lat_send, lat_recv, f_send, f_recv, b_send, b_recv, y_sem):
    my_tp = lax.axis_index('tp')
    my_ctx = lax.axis_index('ctx')
    n_rows, n_cols = y_ref.shape
    heads = o_ref.shape[1] // VALUE
    groups = heads // GROUP
    q_rank = cq.shape[1]
    lat_rank = wkv.shape[2]
    n_keys = 2 * CTX * PIECE
    low_keys = CTX * PIECE
    n_down = 1 + q_rank // DOWN_BLK
    left = lax.rem(my_tp + TP - 1, TP)
    right = lax.rem(my_tp + 1, TP)
    partner = my_ctx + 1 - 2 * lax.rem(my_ctx, 2)
    across = lax.rem(my_ctx + 2, CTX)

    x_copy = pltpu.make_async_copy(x_hbm, x_ref, x_sem)
    kr_copy = pltpu.make_async_copy(wkr_hbm, wkr_ref, kr_sem)

    def dq_copy(blk):
        cols = pl.ds(pl.multiple_of((blk - 1) * DOWN_BLK, DOWN_BLK), DOWN_BLK)
        slot = lax.rem(blk, O_SLOTS)
        return pltpu.make_async_copy(wdq_hbm.at[:, cols], wbig.at[slot], down_sem.at[slot])

    dkv_copy = pltpu.make_async_copy(wdkv_hbm, wbig.at[0], down_sem.at[0])

    def q_copies(grp):
        slot = lax.rem(grp, 2)
        n_blk, r_blk = GROUP * NOPE, GROUP * ROPE
        return (pltpu.make_async_copy(wuq_hbm.at[:, pl.ds(pl.multiple_of(grp * n_blk, n_blk), n_blk)], wq.at[slot], q_sem.at[slot, 0]),
                pltpu.make_async_copy(wqr_hbm.at[:, pl.ds(pl.multiple_of(grp * r_blk, r_blk), r_blk)], wqr.at[slot], q_sem.at[slot, 1]))

    def kv_copies(turn):
        grp, slot = lax.rem(turn, groups), lax.rem(turn, 2)
        n_blk = GROUP * NOPE
        cols = pl.ds(pl.multiple_of(grp * n_blk, n_blk), n_blk)
        return (pltpu.make_async_copy(wuk_hbm.at[:, cols], wkv.at[slot, 0], kv_sem.at[slot, 0]),
                pltpu.make_async_copy(wuv_hbm.at[:, cols], wkv.at[slot, 1], kv_sem.at[slot, 1]))

    row_blks = n_rows // PIECE
    half_cols = n_cols // 2
    col_steps = half_cols // COL_BLK
    n_chunks = col_steps * row_blks

    def o_copies(turn):
        step, slot = lax.rem(turn, col_steps), lax.rem(turn, O_SLOTS)
        return [pltpu.make_async_copy(
            wo_hbm.at[:, pl.ds(pl.multiple_of(side * half_cols + step * COL_BLK, COL_BLK), COL_BLK)],
            wbig.at[slot, pl.ds(0, heads * VALUE), pl.ds(side * COL_BLK, COL_BLK)], o_sem.at[slot, side]) for side in range(2)]

    def start_all(copies):
        for copy in copies:
            copy.start()

    def wait_all(copies):
        for copy in copies:
            copy.wait()

    x_copy.start()
    kr_copy.start()
    dkv_copy.start()
    dq_copy(1).start()
    dq_copy(2).start()

    barrier = pltpu.get_barrier_semaphore()
    for peer in (partner, across):
        pl.semaphore_signal(barrier, inc=1, device_id={'ctx': peer}, device_id_type=MESH_ID)

    @pl.when(my_tp > 0)
    def _():
        pl.semaphore_signal(barrier, inc=1, device_id={'tp': left}, device_id_type=MESH_ID)

    @pl.when(my_tp < TP - 1)
    def _():
        pl.semaphore_signal(barrier, inc=1, device_id={'tp': right}, device_id_type=MESH_ID)

    row = lax.broadcasted_iota(jnp.int32, (n_rows, n_rows), 0)
    col = lax.broadcasted_iota(jnp.int32, (n_rows, n_rows), 1)
    pos_row = pos_ref[...].astype(jnp.float32).reshape(1, n_rows)
    pos_col = jnp.sum(jnp.where(row == col, pos_row, 0.0), axis=1, keepdims=True)
    angles = pos_col * freq_ref[...]
    lane_of = lax.broadcasted_iota(jnp.int32, angles.shape, 1)
    cos_t = jnp.cos(angles)
    sin_t = jnp.where(lax.rem(lane_of, ROPE) < ROPE // 2, -1.0, 1.0) * jnp.sin(angles)
    for copy in range(GROUP // 2):
        cos_ref[:, copy * 2 * ROPE:(copy + 1) * 2 * ROPE] = cos_t
        sin_ref[:, copy * 2 * ROPE:(copy + 1) * 2 * ROPE] = sin_t

    for half, width in ((0, low_keys), (1, n_keys)):
        q_rank_of = (my_ctx if half == 0 else 2 * CTX - 1 - my_ctx) * PIECE + lax.broadcasted_iota(jnp.int32, (PIECE, width), 0)
        key = lax.broadcasted_iota(jnp.int32, (PIECE, width), 1)
        up_piece = 2 * CTX - 1 - (key - low_keys) // PIECE
        k_rank_of = jnp.where(key < low_keys, key, up_piece * PIECE + lax.rem(key, PIECE))
        start = 0 if half == 0 else low_keys
        cap[:, start:start + width] = jnp.where(k_rank_of <= q_rank_of, POS_BIG, NEG_BIG)

    x_copy.wait()
    kr_copy.wait()
    rot = lax.dot_general(x_ref[...], wkr_ref[...], (((1,), (1,)), ((), ())), preferred_element_type=jnp.float32)
    rot = jnp.concatenate([rot, rot], axis=1)
    k_rot = rotate(rot, cos_ref[:, :2 * ROPE], sin_ref[:, :2 * ROPE]).astype(jnp.bfloat16)
    dkv_copy.wait()
    c_kv = rms_norm(jnp.dot(x_ref[...], wbig[0], preferred_element_type=jnp.float32), gkv_ref[...].astype(jnp.float32).reshape(1, lat_rank)).astype(jnp.bfloat16)
    for half in range(2):
        rows = slice(half * PIECE, (half + 1) * PIECE)
        lat[half, my_ctx, :, :lat_rank] = c_kv[rows]
        lat[half, my_ctx, :, lat_rank:] = k_rot[rows]

    @pl.when((my_tp > 0) & (my_tp < TP - 1))
    def _():
        pl.semaphore_wait(barrier, 4)

    @pl.when((my_tp == 0) | (my_tp == TP - 1))
    def _():
        pl.semaphore_wait(barrier, 3)

    def lat_copy(owner, peer, sem):
        part = lat.at[:, owner]
        return pltpu.make_async_remote_copy(src_ref=part, dst_ref=part, send_sem=lat_send.at[sem], recv_sem=lat_recv.at[sem],
                                            device_id={'ctx': peer}, device_id_type=MESH_ID)

    lat_copy(my_ctx, across, 1).start()
    lat_copy(my_ctx, partner, 0).start()

    for blk in range(O_SLOTS, n_down):
        dq_copy(blk).start()
    for grp in range(2):
        start_all(q_copies(grp))

    def dq_step(blk, _):
        dq_copy(blk).wait()
        cols = pl.ds(pl.multiple_of((blk - 1) * DOWN_BLK, DOWN_BLK), DOWN_BLK)
        cq_f[:, cols] = jnp.dot(x_ref[...], wbig[lax.rem(blk, O_SLOTS)], preferred_element_type=jnp.float32)
        return 0

    lax.fori_loop(1, n_down, dq_step, 0)
    cq[...] = rms_norm(cq_f[...], gq_ref[...].astype(jnp.float32).reshape(1, q_rank)).astype(jnp.bfloat16)

    def q_step(grp, _):
        slot = lax.rem(grp, 2)
        wait_all(q_copies(grp))
        qn[grp] = jnp.dot(cq[...], wq[slot], preferred_element_type=jnp.float32).astype(jnp.bfloat16)
        q_rot = jnp.dot(cq[...], wqr[slot], preferred_element_type=jnp.float32)
        qp[grp] = rotate(q_rot, cos_ref[...], sin_ref[...]).astype(jnp.bfloat16)

        @pl.when(grp + 2 < groups)
        def _():
            start_all(q_copies(grp + 2))

        @pl.when(grp + 2 >= groups)
        def _():
            start_all(kv_copies(grp + 2 - groups))

        @pl.when(grp == RELAY_AT)
        def _():
            lat_copy(across, across, 1).wait_recv()
            lat_copy(across, partner, 2).start()
        return 0

    lax.fori_loop(0, groups, q_step, 0)
    lat_copy(partner, partner, 0).wait_recv()
    lat_copy(across, partner, 2).wait_recv()

    lane = lax.broadcasted_iota(jnp.int32, (n_keys, 2 * ROPE), 1)
    k_rots = lat[:, :, :, lat_rank:].reshape(n_keys, 2 * ROPE)
    zero = jnp.zeros_like(k_rots)
    kpe[0] = jnp.where(lane < ROPE, k_rots, zero)
    kpe[1] = jnp.where(lane < ROPE, zero, k_rots)

    expo_scale = (NOPE + ROPE) ** -0.5 * math.log2(math.e)

    def attend(jobs):
        scores = [jnp.minimum(lax.dot_general(q_cat, k_cat, (((1,), (1,)), ((), ())), preferred_element_type=jnp.float32), caps)
                  for q_cat, k_cat, _, caps, _ in jobs]
        tops = [jnp.max(score, axis=-1, keepdims=True) for score in scores]
        probs = [jnp.exp2((score - top) * expo_scale) for score, top in zip(scores, tops)]
        totals = [jnp.sum(prob, axis=-1, keepdims=True) for prob in probs]
        outs = [jnp.dot(prob.astype(jnp.bfloat16), job[2], preferred_element_type=jnp.float32) for prob, job in zip(probs, jobs)]
        for out, total, job in zip(outs, totals, jobs):
            rows, cols = job[4]
            o_ref[rows, cols] = (out / total).astype(jnp.bfloat16)

    def queries(grp, head, rows):
        pair = slice((head // 2) * 2 * ROPE, (head // 2 + 1) * 2 * ROPE)
        return jnp.concatenate([qn[grp, rows, head * NOPE:(head + 1) * NOPE], qp[grp, rows, pair]], axis=1)

    def up_project(half, slot):
        rows = lat[half, :, :, :lat_rank].reshape(low_keys, lat_rank)
        return [jnp.dot(rows, wkv[slot, part], preferred_element_type=jnp.float32).astype(jnp.bfloat16) for part in range(2)]

    def out_cols(grp, head):
        return pl.ds(pl.multiple_of(grp * (GROUP * VALUE), GROUP * VALUE) + head * VALUE, VALUE)

    low, high = slice(0, PIECE), slice(PIECE, 2 * PIECE)

    def low_step(grp, _):
        slot = lax.rem(grp, 2)
        wait_all(kv_copies(grp))
        k_low, v_low = up_project(0, slot)
        kv_low[grp, 0] = k_low
        kv_low[grp, 1] = v_low
        jobs = []
        for head in range(GROUP):
            cols = slice(head * NOPE, (head + 1) * NOPE)
            k_cat = jnp.concatenate([k_low[:, cols], kpe[head % 2, :low_keys]], axis=1)
            jobs.append((queries(grp, head, low), k_cat, v_low[:, cols], cap[:, :low_keys], (low, out_cols(grp, head))))
        for first in range(0, GROUP, LOW_WIDE):
            attend(jobs[first:first + LOW_WIDE])
        start_all(kv_copies(grp + 2))

        @pl.when((grp >= 1) & (grp < O_SLOTS))
        def _():
            start_all(o_copies(grp - 1))
        return 0

    lax.fori_loop(0, groups, low_step, 0)

    def high_step(grp):
        slot = lax.rem(grp, 2)
        wait_all(kv_copies(groups + grp))
        k_up, v_up = up_project(1, slot)
        jobs = []
        for head in range(GROUP):
            cols = slice(head * NOPE, (head + 1) * NOPE)
            keys = jnp.concatenate([kv_low[grp, 0, :, cols], k_up[:, cols]], axis=0)
            values = jnp.concatenate([kv_low[grp, 1, :, cols], v_up[:, cols]], axis=0)
            k_cat = jnp.concatenate([keys, kpe[head % 2]], axis=1)
            jobs.append((queries(grp, head, high), k_cat, values, cap[:, low_keys:], (high, out_cols(grp, head))))
        for first in range(0, GROUP, HIGH_WIDE):
            attend(jobs[first:first + HIGH_WIDE])

        @pl.when(grp + 2 < groups)
        def _():
            start_all(kv_copies(groups + grp + 2))

    depth = (TP - 1 - my_tp, my_tp)
    onward = (left, right)
    back = (right, left)

    def y_slice(side, chunk):
        row, step = chunk // col_steps, lax.rem(chunk, col_steps)
        return (pl.ds(pl.multiple_of(row * PIECE, PIECE), PIECE),
                pl.ds(pl.multiple_of(side * half_cols + step * COL_BLK, COL_BLK), COL_BLK))

    def f_copy(side, chunk):
        return pltpu.make_async_remote_copy(
            src_ref=acc.at[side, chunk], dst_ref=rbuf.at[side, chunk],
            send_sem=f_send.at[side, chunk], recv_sem=f_recv.at[side, chunk],
            device_id={'tp': onward[side]}, device_id_type=MESH_ID)

    def b_copy(side, chunk):
        part = y_ref.at[y_slice(side, chunk)]
        return pltpu.make_async_remote_copy(
            src_ref=part, dst_ref=part,
            send_sem=b_send.at[side, chunk], recv_sem=b_recv.at[side, chunk],
            device_id={'tp': back[side]}, device_id_type=MESH_ID)

    def y_copy(side, chunk):
        return pltpu.make_async_copy(y_ref.at[y_slice(side, chunk)], y_hbm.at[y_slice(side, chunk)], y_sem.at[side, chunk])

    def reduce_event(side, event, row):
        chunk = event - SUM_LAG * (depth[side] - 1)
        live = (chunk >= 0) & (chunk < col_steps)
        chunk = chunk + row * col_steps

        @pl.when(live & (depth[side] > 0))
        def _():
            f_copy(side, chunk).wait_recv()

        @pl.when(live & (depth[side] > 0) & (depth[side] < TP - 1))
        def _():
            acc[side, chunk] = acc[side, chunk] + rbuf[side, chunk]
            f_copy(side, chunk).start()

        @pl.when(live & (depth[side] == TP - 1))
        def _():
            total = acc[side, chunk] + rbuf[side, chunk]
            y_ref[y_slice(side, chunk)] = total.astype(y_ref.dtype)
            b_copy(side, chunk).start()
            y_copy(side, chunk).start()

    def back_event(side, event, row):
        chunk = event - BACK_LAG[row] * (TP - 2 - depth[side])
        live = (chunk >= 0) & (chunk < col_steps)
        chunk = chunk + row * col_steps

        @pl.when(live & (depth[side] < TP - 1))
        def _():
            b_copy(side, chunk).wait_recv()

        @pl.when(live & (depth[side] > 0) & (depth[side] < TP - 1))
        def _():
            b_copy(side, chunk).start()

        @pl.when(live & (depth[side] < TP - 1))
        def _():
            y_copy(side, chunk).start()

    def both(event_fn, event, row):
        for side in range(2):
            event_fn(side, event, row)

    def project(row, step):
        turn = row * col_steps + step

        @pl.when(turn + O_SLOTS - 1 < row_blks * col_steps)
        def _():
            start_all(o_copies(turn + O_SLOTS - 1))

        wait_all(o_copies(turn))
        part = jnp.dot(o_ref[row * PIECE:(row + 1) * PIECE], wbig[lax.rem(turn, O_SLOTS), :heads * VALUE], preferred_element_type=jnp.float32)
        for side in range(2):
            acc[side, turn] = part[:, side * COL_BLK:(side + 1) * COL_BLK]

            @pl.when(depth[side] == 0)
            def _():
                f_copy(side, turn).start()

    sum_events = col_steps + SUM_LAG * (TP - 2)
    back_events = [col_steps + lag * (TP - 2) for lag in BACK_LAG]

    def low_out(step, _):
        project(0, step)

        @pl.when((step >= LOW_FIRST) & (lax.rem(step, 2) == 0))
        def _():
            both(reduce_event, (step - LOW_FIRST) // 2, 0)
        return 0

    lax.fori_loop(0, col_steps, low_out, 0)

    def high_attention(grp, _):
        high_step(grp)

        @pl.when(lax.rem(grp, 4) != 3)
        def _():
            both(reduce_event, EVENTS_OUT + grp - grp // 4, 0)
        return 0

    lax.fori_loop(0, groups, high_attention, 0)

    first_sum = EVENTS_OUT + groups - groups // 4

    def high_out(step, _):
        project(1, step)

        @pl.when((lax.rem(step, 2) == 0) & (first_sum + step // 2 < sum_events))
        def _():
            both(reduce_event, first_sum + step // 2, 0)

        @pl.when((step >= HIGH_FIRST) & (lax.rem(step, 2) == 1))
        def _():
            both(back_event, (step - HIGH_FIRST) // 2, 0)
        return 0

    lax.fori_loop(0, col_steps, high_out, 0)

    first_back = (col_steps - HIGH_FIRST + 1) // 2

    def high_sum(event, _):
        @pl.when(lax.rem(event, 2) == 1)
        def _():
            both(back_event, first_back + EXTRA + event // 2, 0)

        both(reduce_event, event, 1)
        return 0

    for event in range(EXTRA):
        both(back_event, first_back + event, 0)
    lax.fori_loop(0, sum_events, high_sum, 0)
    for event in range(first_back + EXTRA + sum_events // 2, back_events[0]):
        both(back_event, event, 0)

    def high_back(event, _):
        both(back_event, event, 1)
        return 0

    lax.fori_loop(0, back_events[1], high_back, 0)

    lat_copy(my_ctx, partner, 0).wait_send()
    lat_copy(my_ctx, across, 1).wait_send()
    lat_copy(across, partner, 2).wait_send()

    def drain(chunk, _):
        for side in range(2):
            @pl.when(depth[side] < TP - 1)
            def _():
                f_copy(side, chunk).wait_send()

            @pl.when(depth[side] > 0)
            def _():
                b_copy(side, chunk).wait_send()

            y_copy(side, chunk).wait()
        return 0

    lax.fori_loop(0, n_chunks, drain, 0)


def layer(tok_x, tok_pos, w_dq, g_q, w_uq, w_qr, w_dkv, g_kv, w_kr, w_uk, w_uv, w_o):
    n_rows, model_dim = tok_x.shape
    q_rank, lat_rank = w_dq.shape[1], w_dkv.shape[1]
    heads = w_uq.shape[1] // NOPE
    groups = heads // GROUP
    n_keys = CTX * n_rows
    n_chunks = (model_dim // 2 // COL_BLK) * (n_rows // PIECE)
    bf16, f32 = jnp.bfloat16, jnp.float32
    vmem = pl.BlockSpec(memory_space=pltpu.VMEM)
    hbm = pl.BlockSpec(memory_space=pl.ANY)
    dma = pltpu.SemaphoreType.DMA
    return pl.pallas_call(
        layer_kernel,
        out_shape=jax.ShapeDtypeStruct((n_rows, model_dim), bf16),
        in_specs=[hbm, vmem, vmem, vmem, vmem] + [hbm] * 8,
        out_specs=hbm,
        scratch_shapes=[
            pltpu.VMEM((n_rows, model_dim), bf16),
            pltpu.VMEM((n_rows, model_dim), bf16),
            pltpu.VMEM((ROPE, model_dim), bf16),
            pltpu.VMEM((O_SLOTS, model_dim, DOWN_BLK), bf16),
            pltpu.VMEM((2, q_rank, GROUP * NOPE), bf16),
            pltpu.VMEM((2, q_rank, GROUP * ROPE), bf16),
            pltpu.VMEM((2, 2, lat_rank, GROUP * NOPE), bf16),
            pltpu.VMEM((n_rows, GROUP * ROPE), f32),
            pltpu.VMEM((n_rows, GROUP * ROPE), f32),
            pltpu.VMEM((2, CTX, PIECE, lat_rank + 2 * ROPE), bf16),
            pltpu.VMEM((2, n_keys, 2 * ROPE), bf16),
            pltpu.VMEM((n_rows, q_rank), f32),
            pltpu.VMEM((n_rows, q_rank), bf16),
            pltpu.VMEM((groups, n_rows, GROUP * NOPE), bf16),
            pltpu.VMEM((groups, n_rows, GROUP * ROPE), bf16),
            pltpu.VMEM((groups, 2, n_keys // 2, GROUP * NOPE), bf16),
            pltpu.VMEM((PIECE, n_keys // 2 + n_keys), f32),
            pltpu.VMEM((n_rows, heads * VALUE), bf16),
            pltpu.VMEM((2, n_chunks, PIECE, COL_BLK), f32),
            pltpu.VMEM((2, n_chunks, PIECE, COL_BLK), f32),
            dma, dma, dma((O_SLOTS,)), dma((2, 2)), dma((2, 2)), dma((O_SLOTS, 2)),
            dma((3,)), dma((3,)),
            dma((2, n_chunks)), dma((2, n_chunks)), dma((2, n_chunks)), dma((2, n_chunks)), dma((2, n_chunks)),
        ],
        compiler_params=pltpu.CompilerParams(collective_id=0, has_side_effects=True, vmem_limit_bytes=67043328),
        name='layer',
    )(tok_x, tok_pos, jnp.asarray(inv_freq_row()), g_q, g_kv, w_dq, w_uq, w_qr, w_dkv, w_kr.T, w_uk, w_uv, w_o)


def solution(mesh):
    tok_spec = P(('dp', 'ctx'), None)
    pos_spec = P(('dp', 'ctx'))
    full_mat = P(None, None)
    full_vec = P(None)
    col_spec = P(None, 'tp')
    row_spec = P('tp', None)
    return jax.shard_map(layer, mesh=mesh,
                         in_specs=(tok_spec, pos_spec, full_mat, full_vec, col_spec, col_spec, full_mat, full_vec, full_mat, col_spec, col_spec, row_spec),
                         out_specs=tok_spec, check_vma=False)
```

```python
import math

import jax
import jax.numpy as jnp
import numpy as np
from jax import lax
from jax.experimental import pallas as pl
from jax.experimental.pallas import tpu as pltpu
from jax.sharding import PartitionSpec as P

ROPE_BASE = 10000.0
NORM_EPS = 1e-6
NEG_BIG = -1e30
POS_BIG = 3e38
TP = 4
CTX = 4
PIECE = 128
NOPE = 128
ROPE = 64
VALUE = 128
GROUP = 4
DOWN_BLK = 512
COL_BLK = 256
O_SLOTS = 3
LOW_FIRST = 4
HIGH_FIRST = 5
EVENTS_OUT = 3
RELAY_AT = 1
Q_AHEAD = 3
O_AT = 3
EXTRA = 0
HIGH_WIDE = 2
SUM_LAG = 2
BACK_LAG = (1, 3)
MESH_ID = pl.DeviceIdType.MESH


def inv_freq_row():
    half_dim = ROPE // 2
    inv_freq = np.float32(ROPE_BASE) ** (-np.arange(half_dim, dtype=np.float32) * np.float32(2.0) / np.float32(ROPE))
    return np.tile(inv_freq.astype(np.float32), 4)[None]


def rms_norm(act_in, gain_row):
    inv_rms = lax.rsqrt(jnp.mean(act_in * act_in, axis=-1, keepdims=True) + NORM_EPS)
    return act_in * inv_rms * gain_row


def rotate(rows, cos_t, sin_t):
    width = rows.shape[1]
    lane = lax.broadcasted_iota(jnp.int32, rows.shape, 1)
    swapped = jnp.where(lax.rem(lane, ROPE) < ROPE // 2,
                        pltpu.roll(rows, width - ROPE // 2, 1), pltpu.roll(rows, ROPE // 2, 1))
    return rows * cos_t + swapped * sin_t


def layer_kernel(x_hbm, pos_ref, freq_ref, gq_ref, gkv_ref, wdq_hbm, wuq_hbm, wqr_hbm, wdkv_hbm, wkr_hbm, wuk_hbm, wuv_hbm, wo_hbm,
                 y_hbm,
                 y_ref, x_ref, wkr_ref, wbig, wq, wqr, wkv,
                 cos_ref, sin_ref, lat, kpe, cq_f, cq, qn, qp, kv_low, cap, o_ref, acc, rbuf,
                 x_sem, kr_sem, down_sem, q_sem, kv_sem, o_sem,
                 lat_send, lat_recv, f_send, f_recv, b_send, b_recv, y_sem):
    my_tp = lax.axis_index('tp')
    my_ctx = lax.axis_index('ctx')
    n_rows, n_cols = y_ref.shape
    heads = o_ref.shape[1] // VALUE
    groups = heads // GROUP
    q_rank = cq.shape[1]
    lat_rank = wkv.shape[2]
    n_keys = 2 * CTX * PIECE
    low_keys = CTX * PIECE
    n_down = 1 + q_rank // DOWN_BLK
    left = lax.rem(my_tp + TP - 1, TP)
    right = lax.rem(my_tp + 1, TP)
    partner = my_ctx + 1 - 2 * lax.rem(my_ctx, 2)
    across = lax.rem(my_ctx + 2, CTX)

    x_copy = pltpu.make_async_copy(x_hbm, x_ref, x_sem)
    kr_copy = pltpu.make_async_copy(wkr_hbm, wkr_ref, kr_sem)

    def dq_copy(blk):
        cols = pl.ds(pl.multiple_of((blk - 1) * DOWN_BLK, DOWN_BLK), DOWN_BLK)
        slot = lax.rem(blk, O_SLOTS)
        return pltpu.make_async_copy(wdq_hbm.at[:, cols], wbig.at[slot], down_sem.at[slot])

    dkv_copy = pltpu.make_async_copy(wdkv_hbm, wbig.at[0], down_sem.at[0])

    def q_copies(grp):
        slot = lax.rem(grp, 2)
        n_blk, r_blk = GROUP * NOPE, GROUP * ROPE
        return (pltpu.make_async_copy(wuq_hbm.at[:, pl.ds(pl.multiple_of(grp * n_blk, n_blk), n_blk)], wq.at[slot], q_sem.at[slot, 0]),
                pltpu.make_async_copy(wqr_hbm.at[:, pl.ds(pl.multiple_of(grp * r_blk, r_blk), r_blk)], wqr.at[slot], q_sem.at[slot, 1]))

    def kv_copies(turn):
        grp, slot = lax.rem(turn, groups), lax.rem(turn, 2)
        n_blk = GROUP * NOPE
        cols = pl.ds(pl.multiple_of(grp * n_blk, n_blk), n_blk)
        return (pltpu.make_async_copy(wuk_hbm.at[:, cols], wkv.at[slot, 0], kv_sem.at[slot, 0]),
                pltpu.make_async_copy(wuv_hbm.at[:, cols], wkv.at[slot, 1], kv_sem.at[slot, 1]))

    row_blks = n_rows // PIECE
    half_cols = n_cols // 2
    col_steps = half_cols // COL_BLK
    n_chunks = col_steps * row_blks

    def o_copies(turn):
        step, slot = lax.rem(turn, col_steps), lax.rem(turn, O_SLOTS)
        return [pltpu.make_async_copy(
            wo_hbm.at[:, pl.ds(pl.multiple_of(side * half_cols + step * COL_BLK, COL_BLK), COL_BLK)],
            wbig.at[slot, pl.ds(0, heads * VALUE), pl.ds(side * COL_BLK, COL_BLK)], o_sem.at[slot, side]) for side in range(2)]

    def start_all(copies):
        for copy in copies:
            copy.start()

    def wait_all(copies):
        for copy in copies:
            copy.wait()

    x_copy.start()
    kr_copy.start()
    dkv_copy.start()

    barrier = pltpu.get_barrier_semaphore()
    for peer in (partner, across):
        pl.semaphore_signal(barrier, inc=1, device_id={'ctx': peer}, device_id_type=MESH_ID)

    @pl.when(my_tp > 0)
    def _():
        pl.semaphore_signal(barrier, inc=1, device_id={'tp': left}, device_id_type=MESH_ID)

    @pl.when(my_tp < TP - 1)
    def _():
        pl.semaphore_signal(barrier, inc=1, device_id={'tp': right}, device_id_type=MESH_ID)

    row = lax.broadcasted_iota(jnp.int32, (n_rows, n_rows), 0)
    col = lax.broadcasted_iota(jnp.int32, (n_rows, n_rows), 1)
    pos_row = pos_ref[...].astype(jnp.float32).reshape(1, n_rows)
    pos_col = jnp.sum(jnp.where(row == col, pos_row, 0.0), axis=1, keepdims=True)
    angles = pos_col * freq_ref[...]
    lane_of = lax.broadcasted_iota(jnp.int32, angles.shape, 1)
    cos_t = jnp.cos(angles)
    sin_t = jnp.where(lax.rem(lane_of, ROPE) < ROPE // 2, -1.0, 1.0) * jnp.sin(angles)
    for copy in range(GROUP // 2):
        cos_ref[:, copy * 2 * ROPE:(copy + 1) * 2 * ROPE] = cos_t
        sin_ref[:, copy * 2 * ROPE:(copy + 1) * 2 * ROPE] = sin_t

    for half, width in ((0, low_keys), (1, n_keys)):
        q_rank_of = (my_ctx if half == 0 else 2 * CTX - 1 - my_ctx) * PIECE + lax.broadcasted_iota(jnp.int32, (PIECE, width), 0)
        key = lax.broadcasted_iota(jnp.int32, (PIECE, width), 1)
        up_piece = 2 * CTX - 1 - (key - low_keys) // PIECE
        k_rank_of = jnp.where(key < low_keys, key, up_piece * PIECE + lax.rem(key, PIECE))
        start = 0 if half == 0 else low_keys
        cap[:, start:start + width] = jnp.where(k_rank_of <= q_rank_of, POS_BIG, NEG_BIG)

    x_copy.wait()
    kr_copy.wait()
    dq_copy(1).start()
    rot = lax.dot_general(x_ref[...], wkr_ref[...], (((1,), (1,)), ((), ())), preferred_element_type=jnp.float32)
    rot = jnp.concatenate([rot, rot], axis=1)
    k_rot = rotate(rot, cos_ref[:, :2 * ROPE], sin_ref[:, :2 * ROPE]).astype(jnp.bfloat16)
    dkv_copy.wait()
    dq_copy(2).start()
    c_kv = rms_norm(jnp.dot(x_ref[...], wbig[0], preferred_element_type=jnp.float32), gkv_ref[...].astype(jnp.float32).reshape(1, lat_rank)).astype(jnp.bfloat16)
    for half in range(2):
        rows = slice(half * PIECE, (half + 1) * PIECE)
        lat[half, my_ctx, :, :lat_rank] = c_kv[rows]
        lat[half, my_ctx, :, lat_rank:] = k_rot[rows]

    @pl.when((my_tp > 0) & (my_tp < TP - 1))
    def _():
        pl.semaphore_wait(barrier, 4)

    @pl.when((my_tp == 0) | (my_tp == TP - 1))
    def _():
        pl.semaphore_wait(barrier, 3)

    def lat_copy(owner, peer, sem):
        part = lat.at[:, owner]
        return pltpu.make_async_remote_copy(src_ref=part, dst_ref=part, send_sem=lat_send.at[sem], recv_sem=lat_recv.at[sem],
                                            device_id={'ctx': peer}, device_id_type=MESH_ID)

    lat_copy(my_ctx, across, 1).start()
    lat_copy(my_ctx, partner, 0).start()

    for blk in range(O_SLOTS, n_down):
        dq_copy(blk).start()
    for grp in range(2):
        start_all(q_copies(grp))

    def dq_step(blk, _):
        dq_copy(blk).wait()
        cols = pl.ds(pl.multiple_of((blk - 1) * DOWN_BLK, DOWN_BLK), DOWN_BLK)
        cq_f[:, cols] = jnp.dot(x_ref[...], wbig[lax.rem(blk, O_SLOTS)], preferred_element_type=jnp.float32)
        return 0

    lax.fori_loop(1, n_down, dq_step, 0)
    cq[...] = rms_norm(cq_f[...], gq_ref[...].astype(jnp.float32).reshape(1, q_rank)).astype(jnp.bfloat16)

    def q_project(grp):
        slot = lax.rem(grp, 2)
        qn[grp] = jnp.dot(cq[...], wq[slot], preferred_element_type=jnp.float32).astype(jnp.bfloat16)
        q_rot = jnp.dot(cq[...], wqr[slot], preferred_element_type=jnp.float32)
        qp[grp] = rotate(q_rot, cos_ref[...], sin_ref[...]).astype(jnp.bfloat16)

    def q_step(grp, _):
        wait_all(q_copies(grp))
        q_project(grp)
        start_all(q_copies(grp + 2))

        @pl.when(grp < 2)
        def _():
            start_all(kv_copies(grp))

        @pl.when(grp == RELAY_AT)
        def _():
            lat_copy(across, across, 1).wait_recv()
            lat_copy(across, partner, 2).start()
        return 0

    lax.fori_loop(0, Q_AHEAD, q_step, 0)
    lat_copy(partner, partner, 0).wait_recv()
    lat_copy(across, partner, 2).wait_recv()

    lane = lax.broadcasted_iota(jnp.int32, (n_keys, 2 * ROPE), 1)
    k_rots = lat[:, :, :, lat_rank:].reshape(n_keys, 2 * ROPE)
    zero = jnp.zeros_like(k_rots)
    kpe[0] = jnp.where(lane < ROPE, k_rots, zero)
    kpe[1] = jnp.where(lane < ROPE, zero, k_rots)

    expo_scale = (NOPE + ROPE) ** -0.5 * math.log2(math.e)

    def attend(jobs, between):
        scores = [jnp.minimum(lax.dot_general(q_cat, k_cat, (((1,), (1,)), ((), ())), preferred_element_type=jnp.float32), caps)
                  for q_cat, k_cat, _, caps, _ in jobs]
        between()
        tops = [jnp.max(score, axis=-1, keepdims=True) for score in scores]
        probs = [jnp.exp2((score - top) * expo_scale) for score, top in zip(scores, tops)]
        totals = [jnp.sum(prob, axis=-1, keepdims=True) for prob in probs]
        outs = [jnp.dot(prob.astype(jnp.bfloat16), job[2], preferred_element_type=jnp.float32) for prob, job in zip(probs, jobs)]
        for out, total, job in zip(outs, totals, jobs):
            rows, cols = job[4]
            o_ref[rows, cols] = (out / total).astype(jnp.bfloat16)

    def queries(grp, head, rows):
        pair = slice((head // 2) * 2 * ROPE, (head // 2 + 1) * 2 * ROPE)
        return jnp.concatenate([qn[grp, rows, head * NOPE:(head + 1) * NOPE], qp[grp, rows, pair]], axis=1)

    def up_project(half, slot):
        rows = lat[half, :, :, :lat_rank].reshape(low_keys, lat_rank)
        return [jnp.dot(rows, wkv[slot, part], preferred_element_type=jnp.float32).astype(jnp.bfloat16) for part in range(2)]

    def out_cols(grp, head):
        return pl.ds(pl.multiple_of(grp * (GROUP * VALUE), GROUP * VALUE) + head * VALUE, VALUE)

    low, high = slice(0, PIECE), slice(PIECE, 2 * PIECE)

    def low_step(grp, ahead):
        slot = lax.rem(grp, 2)
        wait_all(kv_copies(grp))
        if ahead:
            wait_all(q_copies(grp + Q_AHEAD))
        k_low, v_low = up_project(0, slot)
        kv_low[grp, 0] = k_low
        kv_low[grp, 1] = v_low
        jobs = []
        for head in range(GROUP):
            cols = slice(head * NOPE, (head + 1) * NOPE)
            k_cat = jnp.concatenate([k_low[:, cols], kpe[head % 2, :low_keys]], axis=1)
            jobs.append((queries(grp, head, low), k_cat, v_low[:, cols], cap[:, :low_keys], (low, out_cols(grp, head))))
        attend(jobs, (lambda: q_project(grp + Q_AHEAD)) if ahead else (lambda: None))
        start_all(kv_copies(grp + 2))
        if ahead:
            @pl.when(grp + Q_AHEAD + 2 < groups)
            def _():
                start_all(q_copies(grp + Q_AHEAD + 2))

        @pl.when((grp >= O_AT) & (grp < O_AT + O_SLOTS - 1))
        def _():
            start_all(o_copies(grp - O_AT))

    def low_ahead(grp, _):
        low_step(grp, True)
        return 0

    def low_rest(grp, _):
        low_step(grp, False)
        return 0

    lax.fori_loop(0, groups - Q_AHEAD, low_ahead, 0)
    lax.fori_loop(groups - Q_AHEAD, groups, low_rest, 0)

    def high_step(grp):
        slot = lax.rem(grp, 2)
        wait_all(kv_copies(groups + grp))
        k_up, v_up = up_project(1, slot)
        jobs = []
        for head in range(GROUP):
            cols = slice(head * NOPE, (head + 1) * NOPE)
            keys = jnp.concatenate([kv_low[grp, 0, :, cols], k_up[:, cols]], axis=0)
            values = jnp.concatenate([kv_low[grp, 1, :, cols], v_up[:, cols]], axis=0)
            k_cat = jnp.concatenate([keys, kpe[head % 2]], axis=1)
            jobs.append((queries(grp, head, high), k_cat, values, cap[:, low_keys:], (high, out_cols(grp, head))))
        for first in range(0, GROUP, HIGH_WIDE):
            attend(jobs[first:first + HIGH_WIDE], lambda: None)

        @pl.when(grp + 2 < groups)
        def _():
            start_all(kv_copies(groups + grp + 2))

    depth = (TP - 1 - my_tp, my_tp)
    onward = (left, right)
    back = (right, left)

    def y_slice(side, chunk):
        row, step = chunk // col_steps, lax.rem(chunk, col_steps)
        return (pl.ds(pl.multiple_of(row * PIECE, PIECE), PIECE),
                pl.ds(pl.multiple_of(side * half_cols + step * COL_BLK, COL_BLK), COL_BLK))

    def f_copy(side, chunk):
        return pltpu.make_async_remote_copy(
            src_ref=acc.at[side, chunk], dst_ref=rbuf.at[side, chunk],
            send_sem=f_send.at[side, chunk], recv_sem=f_recv.at[side, chunk],
            device_id={'tp': onward[side]}, device_id_type=MESH_ID)

    def b_copy(side, chunk):
        part = y_ref.at[y_slice(side, chunk)]
        return pltpu.make_async_remote_copy(
            src_ref=part, dst_ref=part,
            send_sem=b_send.at[side, chunk], recv_sem=b_recv.at[side, chunk],
            device_id={'tp': back[side]}, device_id_type=MESH_ID)

    def y_copy(side, chunk):
        return pltpu.make_async_copy(y_ref.at[y_slice(side, chunk)], y_hbm.at[y_slice(side, chunk)], y_sem.at[side, chunk])

    def reduce_event(side, event, row):
        chunk = event - SUM_LAG * (depth[side] - 1)
        live = (chunk >= 0) & (chunk < col_steps)
        chunk = chunk + row * col_steps

        @pl.when(live & (depth[side] > 0))
        def _():
            f_copy(side, chunk).wait_recv()

        @pl.when(live & (depth[side] > 0) & (depth[side] < TP - 1))
        def _():
            acc[side, chunk] = acc[side, chunk] + rbuf[side, chunk]
            f_copy(side, chunk).start()

        @pl.when(live & (depth[side] == TP - 1))
        def _():
            total = acc[side, chunk] + rbuf[side, chunk]
            y_ref[y_slice(side, chunk)] = total.astype(y_ref.dtype)
            b_copy(side, chunk).start()
            y_copy(side, chunk).start()

    def back_event(side, event, row):
        chunk = event - BACK_LAG[row] * (TP - 2 - depth[side])
        live = (chunk >= 0) & (chunk < col_steps)
        chunk = chunk + row * col_steps

        @pl.when(live & (depth[side] < TP - 1))
        def _():
            b_copy(side, chunk).wait_recv()

        @pl.when(live & (depth[side] > 0) & (depth[side] < TP - 1))
        def _():
            b_copy(side, chunk).start()

        @pl.when(live & (depth[side] < TP - 1))
        def _():
            y_copy(side, chunk).start()

    def both(event_fn, event, row):
        for side in range(2):
            event_fn(side, event, row)

    def project(row, step):
        turn = row * col_steps + step

        @pl.when(turn + O_SLOTS - 1 < row_blks * col_steps)
        def _():
            start_all(o_copies(turn + O_SLOTS - 1))

        wait_all(o_copies(turn))
        part = jnp.dot(o_ref[row * PIECE:(row + 1) * PIECE], wbig[lax.rem(turn, O_SLOTS), :heads * VALUE], preferred_element_type=jnp.float32)
        for side in range(2):
            acc[side, turn] = part[:, side * COL_BLK:(side + 1) * COL_BLK]

            @pl.when(depth[side] == 0)
            def _():
                f_copy(side, turn).start()

    sum_events = col_steps + SUM_LAG * (TP - 2)
    back_events = [col_steps + lag * (TP - 2) for lag in BACK_LAG]

    def low_out(step, _):
        project(0, step)

        @pl.when((step >= LOW_FIRST) & (lax.rem(step, 2) == 0))
        def _():
            both(reduce_event, (step - LOW_FIRST) // 2, 0)
        return 0

    lax.fori_loop(0, col_steps, low_out, 0)

    def high_attention(grp, _):
        high_step(grp)

        @pl.when(lax.rem(grp, 4) != 3)
        def _():
            both(reduce_event, EVENTS_OUT + grp - grp // 4, 0)
        return 0

    lax.fori_loop(0, groups, high_attention, 0)

    first_sum = EVENTS_OUT + groups - groups // 4

    def high_out(step, _):
        project(1, step)

        @pl.when((lax.rem(step, 2) == 0) & (first_sum + step // 2 < sum_events))
        def _():
            both(reduce_event, first_sum + step // 2, 0)

        @pl.when((step >= HIGH_FIRST) & (lax.rem(step, 2) == 1))
        def _():
            both(back_event, (step - HIGH_FIRST) // 2, 0)
        return 0

    lax.fori_loop(0, col_steps, high_out, 0)

    first_back = (col_steps - HIGH_FIRST + 1) // 2

    def high_sum(event, _):
        @pl.when(lax.rem(event, 2) == 1)
        def _():
            both(back_event, first_back + EXTRA + event // 2, 0)

        both(reduce_event, event, 1)
        return 0

    for event in range(EXTRA):
        both(back_event, first_back + event, 0)
    lax.fori_loop(0, sum_events, high_sum, 0)
    for event in range(first_back + EXTRA + sum_events // 2, back_events[0]):
        both(back_event, event, 0)

    def high_back(event, _):
        both(back_event, event, 1)
        return 0

    lax.fori_loop(0, back_events[1], high_back, 0)

    lat_copy(my_ctx, partner, 0).wait_send()
    lat_copy(my_ctx, across, 1).wait_send()
    lat_copy(across, partner, 2).wait_send()

    def drain(chunk, _):
        for side in range(2):
            @pl.when(depth[side] < TP - 1)
            def _():
                f_copy(side, chunk).wait_send()

            @pl.when(depth[side] > 0)
            def _():
                b_copy(side, chunk).wait_send()

            y_copy(side, chunk).wait()
        return 0

    lax.fori_loop(0, n_chunks, drain, 0)


def layer(tok_x, tok_pos, w_dq, g_q, w_uq, w_qr, w_dkv, g_kv, w_kr, w_uk, w_uv, w_o):
    n_rows, model_dim = tok_x.shape
    q_rank, lat_rank = w_dq.shape[1], w_dkv.shape[1]
    heads = w_uq.shape[1] // NOPE
    groups = heads // GROUP
    n_keys = CTX * n_rows
    n_chunks = (model_dim // 2 // COL_BLK) * (n_rows // PIECE)
    bf16, f32 = jnp.bfloat16, jnp.float32
    vmem = pl.BlockSpec(memory_space=pltpu.VMEM)
    hbm = pl.BlockSpec(memory_space=pl.ANY)
    dma = pltpu.SemaphoreType.DMA
    return pl.pallas_call(
        layer_kernel,
        out_shape=jax.ShapeDtypeStruct((n_rows, model_dim), bf16),
        in_specs=[hbm, vmem, vmem, vmem, vmem] + [hbm] * 8,
        out_specs=hbm,
        scratch_shapes=[
            pltpu.VMEM((n_rows, model_dim), bf16),
            pltpu.VMEM((n_rows, model_dim), bf16),
            pltpu.VMEM((ROPE, model_dim), bf16),
            pltpu.VMEM((O_SLOTS, model_dim, DOWN_BLK), bf16),
            pltpu.VMEM((2, q_rank, GROUP * NOPE), bf16),
            pltpu.VMEM((2, q_rank, GROUP * ROPE), bf16),
            pltpu.VMEM((2, 2, lat_rank, GROUP * NOPE), bf16),
            pltpu.VMEM((n_rows, GROUP * ROPE), f32),
            pltpu.VMEM((n_rows, GROUP * ROPE), f32),
            pltpu.VMEM((2, CTX, PIECE, lat_rank + 2 * ROPE), bf16),
            pltpu.VMEM((2, n_keys, 2 * ROPE), bf16),
            pltpu.VMEM((n_rows, q_rank), f32),
            pltpu.VMEM((n_rows, q_rank), bf16),
            pltpu.VMEM((groups, n_rows, GROUP * NOPE), bf16),
            pltpu.VMEM((groups, n_rows, GROUP * ROPE), bf16),
            pltpu.VMEM((groups, 2, n_keys // 2, GROUP * NOPE), bf16),
            pltpu.VMEM((PIECE, n_keys // 2 + n_keys), f32),
            pltpu.VMEM((n_rows, heads * VALUE), bf16),
            pltpu.VMEM((2, n_chunks, PIECE, COL_BLK), f32),
            pltpu.VMEM((2, n_chunks, PIECE, COL_BLK), f32),
            dma, dma, dma((O_SLOTS,)), dma((2, 2)), dma((2, 2)), dma((O_SLOTS, 2)),
            dma((3,)), dma((3,)),
            dma((2, n_chunks)), dma((2, n_chunks)), dma((2, n_chunks)), dma((2, n_chunks)), dma((2, n_chunks)),
        ],
        compiler_params=pltpu.CompilerParams(collective_id=0, has_side_effects=True, vmem_limit_bytes=67043328),
        name='layer',
    )(tok_x, tok_pos, jnp.asarray(inv_freq_row()), g_q, g_kv, w_dq, w_uq, w_qr, w_dkv, w_kr.T, w_uk, w_uv, w_o)


def solution(mesh):
    tok_spec = P(('dp', 'ctx'), None)
    pos_spec = P(('dp', 'ctx'))
    full_mat = P(None, None)
    full_vec = P(None)
    col_spec = P(None, 'tp')
    row_spec = P('tp', None)
    return jax.shard_map(layer, mesh=mesh,
                         in_specs=(tok_spec, pos_spec, full_mat, full_vec, col_spec, col_spec, full_mat, full_vec, full_mat, col_spec, col_spec, row_spec),
                         out_specs=tok_spec, check_vma=False)
```

```python
import math

import jax
import jax.numpy as jnp
import numpy as np
from jax import lax
from jax.experimental import pallas as pl
from jax.experimental.pallas import tpu as pltpu
from jax.sharding import PartitionSpec as P

ROPE_BASE = 10000.0
NORM_EPS = 1e-6
NEG_BIG = -1e30
POS_BIG = 3e38
TP = 4
CTX = 4
PIECE = 128
SPLIT = 1
NOPE = 128
ROPE = 64
VALUE = 128
GROUP = 4
DOWN_BLK = 512
COL_BLK = 256
O_SLOTS = 3
LOW_FIRST = 4
HIGH_FIRST = 5
EVENTS_OUT = 3
RELAY_AT = 1
Q_AHEAD = 3
O_AT = 3
STORE_SLABS = 8
EXTRA = 0
HIGH_WIDE = 2
SUM_LAG = 3
BACK_LAG = (1, 4)
MESH_ID = pl.DeviceIdType.MESH


def inv_freq_row():
    half_dim = ROPE // 2
    inv_freq = np.float32(ROPE_BASE) ** (-np.arange(half_dim, dtype=np.float32) * np.float32(2.0) / np.float32(ROPE))
    return np.tile(inv_freq.astype(np.float32), 4)[None]


def rms_norm(act_in, gain_row):
    inv_rms = lax.rsqrt(jnp.mean(act_in * act_in, axis=-1, keepdims=True) + NORM_EPS)
    return act_in * inv_rms * gain_row


def rotate(rows, cos_t, sin_t):
    width = rows.shape[1]
    lane = lax.broadcasted_iota(jnp.int32, rows.shape, 1)
    swapped = jnp.where(lax.rem(lane, ROPE) < ROPE // 2,
                        pltpu.roll(rows, width - ROPE // 2, 1), pltpu.roll(rows, ROPE // 2, 1))
    return rows * cos_t + swapped * sin_t


def layer_kernel(x_hbm, pos_ref, freq_ref, gq_ref, gkv_ref, wdq_hbm, wuq_hbm, wqr_hbm, wdkv_hbm, wkr_hbm, wuk_hbm, wuv_hbm, wo_hbm,
                 y_hbm,
                 y_ref, x_ref, wkr_ref, wbig, wq, wqr, wkv,
                 cos_ref, sin_ref, lat, kpe, cq_f, cq, qn, qp, kv_low, cap, o_ref, acc, rbuf,
                 x_sem, kr_sem, down_sem, q_sem, kv_sem, o_sem,
                 lat_send, lat_recv, f_send, f_recv, b_send, b_recv, y_sem):
    my_tp = lax.axis_index('tp')
    my_ctx = lax.axis_index('ctx')
    n_rows, n_cols = y_ref.shape
    heads = o_ref.shape[1] // VALUE
    groups = heads // GROUP
    q_rank = cq.shape[1]
    lat_rank = wkv.shape[2]
    n_keys = 2 * CTX * PIECE
    low_keys = CTX * PIECE
    n_down = 1 + q_rank // DOWN_BLK
    left = lax.rem(my_tp + TP - 1, TP)
    right = lax.rem(my_tp + 1, TP)
    partner = my_ctx + 1 - 2 * lax.rem(my_ctx, 2)
    across = lax.rem(my_ctx + 2, CTX)

    x_copy = pltpu.make_async_copy(x_hbm, x_ref, x_sem)
    kr_copy = pltpu.make_async_copy(wkr_hbm, wkr_ref, kr_sem)

    def dq_copy(blk):
        cols = pl.ds(pl.multiple_of((blk - 1) * DOWN_BLK, DOWN_BLK), DOWN_BLK)
        slot = lax.rem(blk, O_SLOTS)
        return pltpu.make_async_copy(wdq_hbm.at[:, cols], wbig.at[slot], down_sem.at[slot])

    dkv_copy = pltpu.make_async_copy(wdkv_hbm, wbig.at[0], down_sem.at[0])

    def q_copies(grp):
        slot = lax.rem(grp, 2)
        n_blk, r_blk = GROUP * NOPE, GROUP * ROPE
        return (pltpu.make_async_copy(wuq_hbm.at[:, pl.ds(pl.multiple_of(grp * n_blk, n_blk), n_blk)], wq.at[slot], q_sem.at[slot, 0]),
                pltpu.make_async_copy(wqr_hbm.at[:, pl.ds(pl.multiple_of(grp * r_blk, r_blk), r_blk)], wqr.at[slot], q_sem.at[slot, 1]))

    def kv_copies(turn):
        grp, slot = lax.rem(turn, groups), lax.rem(turn, 2)
        n_blk = GROUP * NOPE
        cols = pl.ds(pl.multiple_of(grp * n_blk, n_blk), n_blk)
        return (pltpu.make_async_copy(wuk_hbm.at[:, cols], wkv.at[slot, 0], kv_sem.at[slot, 0]),
                pltpu.make_async_copy(wuv_hbm.at[:, cols], wkv.at[slot, 1], kv_sem.at[slot, 1]))

    row_blks = n_rows // PIECE
    half_cols = n_cols // 2
    col_steps = half_cols // COL_BLK
    n_chunks = col_steps * row_blks * SPLIT
    row_chunks = col_steps * SPLIT
    chunk_rows = PIECE // SPLIT

    def o_copies(turn):
        step, slot = lax.rem(turn, col_steps), lax.rem(turn, O_SLOTS)
        return [pltpu.make_async_copy(
            wo_hbm.at[:, pl.ds(pl.multiple_of(side * half_cols + step * COL_BLK, COL_BLK), COL_BLK)],
            wbig.at[slot, pl.ds(0, heads * VALUE), pl.ds(side * COL_BLK, COL_BLK)], o_sem.at[slot, side]) for side in range(2)]

    def start_all(copies):
        for copy in copies:
            copy.start()

    def wait_all(copies):
        for copy in copies:
            copy.wait()

    x_copy.start()
    kr_copy.start()
    dkv_copy.start()

    barrier = pltpu.get_barrier_semaphore()
    for peer in (partner, across):
        pl.semaphore_signal(barrier, inc=1, device_id={'ctx': peer}, device_id_type=MESH_ID)

    @pl.when(my_tp > 0)
    def _():
        pl.semaphore_signal(barrier, inc=1, device_id={'tp': left}, device_id_type=MESH_ID)

    @pl.when(my_tp < TP - 1)
    def _():
        pl.semaphore_signal(barrier, inc=1, device_id={'tp': right}, device_id_type=MESH_ID)

    row = lax.broadcasted_iota(jnp.int32, (n_rows, n_rows), 0)
    col = lax.broadcasted_iota(jnp.int32, (n_rows, n_rows), 1)
    pos_row = pos_ref[...].astype(jnp.float32).reshape(1, n_rows)
    pos_col = jnp.sum(jnp.where(row == col, pos_row, 0.0), axis=1, keepdims=True)
    angles = pos_col * freq_ref[...]
    lane_of = lax.broadcasted_iota(jnp.int32, angles.shape, 1)
    cos_t = jnp.cos(angles)
    sin_t = jnp.where(lax.rem(lane_of, ROPE) < ROPE // 2, -1.0, 1.0) * jnp.sin(angles)
    for copy in range(GROUP // 2):
        cos_ref[:, copy * 2 * ROPE:(copy + 1) * 2 * ROPE] = cos_t
        sin_ref[:, copy * 2 * ROPE:(copy + 1) * 2 * ROPE] = sin_t

    for half, width in ((0, low_keys), (1, n_keys)):
        q_rank_of = (my_ctx if half == 0 else 2 * CTX - 1 - my_ctx) * PIECE + lax.broadcasted_iota(jnp.int32, (PIECE, width), 0)
        key = lax.broadcasted_iota(jnp.int32, (PIECE, width), 1)
        up_piece = 2 * CTX - 1 - (key - low_keys) // PIECE
        k_rank_of = jnp.where(key < low_keys, key, up_piece * PIECE + lax.rem(key, PIECE))
        start = 0 if half == 0 else low_keys
        cap[:, start:start + width] = jnp.where(k_rank_of <= q_rank_of, POS_BIG, NEG_BIG)

    x_copy.wait()
    kr_copy.wait()
    dq_copy(1).start()
    rot = lax.dot_general(x_ref[...], wkr_ref[...], (((1,), (1,)), ((), ())), preferred_element_type=jnp.float32)
    rot = jnp.concatenate([rot, rot], axis=1)
    k_rot = rotate(rot, cos_ref[:, :2 * ROPE], sin_ref[:, :2 * ROPE]).astype(jnp.bfloat16)
    dkv_copy.wait()
    dq_copy(2).start()
    c_kv = rms_norm(jnp.dot(x_ref[...], wbig[0], preferred_element_type=jnp.float32), gkv_ref[...].astype(jnp.float32).reshape(1, lat_rank)).astype(jnp.bfloat16)
    for half in range(2):
        rows = slice(half * PIECE, (half + 1) * PIECE)
        lat[half, my_ctx, :, :lat_rank] = c_kv[rows]
        lat[half, my_ctx, :, lat_rank:] = k_rot[rows]

    @pl.when((my_tp > 0) & (my_tp < TP - 1))
    def _():
        pl.semaphore_wait(barrier, 4)

    @pl.when((my_tp == 0) | (my_tp == TP - 1))
    def _():
        pl.semaphore_wait(barrier, 3)

    def lat_copy(owner, peer, sem):
        part = lat.at[:, owner]
        return pltpu.make_async_remote_copy(src_ref=part, dst_ref=part, send_sem=lat_send.at[sem], recv_sem=lat_recv.at[sem],
                                            device_id={'ctx': peer}, device_id_type=MESH_ID)

    lat_copy(my_ctx, across, 1).start()
    lat_copy(my_ctx, partner, 0).start()

    for blk in range(O_SLOTS, n_down):
        dq_copy(blk).start()
    for grp in range(2):
        start_all(q_copies(grp))

    def dq_step(blk, _):
        dq_copy(blk).wait()
        cols = pl.ds(pl.multiple_of((blk - 1) * DOWN_BLK, DOWN_BLK), DOWN_BLK)
        cq_f[:, cols] = jnp.dot(x_ref[...], wbig[lax.rem(blk, O_SLOTS)], preferred_element_type=jnp.float32)
        return 0

    lax.fori_loop(1, n_down, dq_step, 0)
    cq[...] = rms_norm(cq_f[...], gq_ref[...].astype(jnp.float32).reshape(1, q_rank)).astype(jnp.bfloat16)

    def q_project(grp):
        slot = lax.rem(grp, 2)
        qn[grp] = jnp.dot(cq[...], wq[slot], preferred_element_type=jnp.float32).astype(jnp.bfloat16)
        q_rot = jnp.dot(cq[...], wqr[slot], preferred_element_type=jnp.float32)
        qp[grp] = rotate(q_rot, cos_ref[...], sin_ref[...]).astype(jnp.bfloat16)

    def q_step(grp, _):
        wait_all(q_copies(grp))
        q_project(grp)
        start_all(q_copies(grp + 2))

        @pl.when(grp < 2)
        def _():
            start_all(kv_copies(grp))

        @pl.when(grp == RELAY_AT)
        def _():
            lat_copy(across, across, 1).wait_recv()
            lat_copy(across, partner, 2).start()
        return 0

    lax.fori_loop(0, Q_AHEAD, q_step, 0)
    lat_copy(partner, partner, 0).wait_recv()
    lat_copy(across, partner, 2).wait_recv()

    lane = lax.broadcasted_iota(jnp.int32, (n_keys, 2 * ROPE), 1)
    k_rots = lat[:, :, :, lat_rank:].reshape(n_keys, 2 * ROPE)
    zero = jnp.zeros_like(k_rots)
    kpe[0] = jnp.where(lane < ROPE, k_rots, zero)
    kpe[1] = jnp.where(lane < ROPE, zero, k_rots)

    expo_scale = (NOPE + ROPE) ** -0.5 * math.log2(math.e)

    def attend(jobs, between):
        scores = [jnp.minimum(lax.dot_general(q_cat, k_cat, (((1,), (1,)), ((), ())), preferred_element_type=jnp.float32), caps)
                  for q_cat, k_cat, _, caps, _ in jobs]
        between()
        tops = [jnp.max(score, axis=-1, keepdims=True) for score in scores]
        probs = [jnp.exp2((score - top) * expo_scale) for score, top in zip(scores, tops)]
        totals = [jnp.sum(prob, axis=-1, keepdims=True) for prob in probs]
        outs = [jnp.dot(prob.astype(jnp.bfloat16), job[2], preferred_element_type=jnp.float32) for prob, job in zip(probs, jobs)]
        for out, total, job in zip(outs, totals, jobs):
            rows, cols = job[4]
            o_ref[rows, cols] = (out / total).astype(jnp.bfloat16)

    def queries(grp, head, rows):
        pair = slice((head // 2) * 2 * ROPE, (head // 2 + 1) * 2 * ROPE)
        return jnp.concatenate([qn[grp, rows, head * NOPE:(head + 1) * NOPE], qp[grp, rows, pair]], axis=1)

    def up_project(half, slot):
        rows = lat[half, :, :, :lat_rank].reshape(low_keys, lat_rank)
        return [jnp.dot(rows, wkv[slot, part], preferred_element_type=jnp.float32).astype(jnp.bfloat16) for part in range(2)]

    def out_cols(grp, head):
        return pl.ds(pl.multiple_of(grp * (GROUP * VALUE), GROUP * VALUE) + head * VALUE, VALUE)

    low, high = slice(0, PIECE), slice(PIECE, 2 * PIECE)

    def low_step(grp, ahead):
        slot = lax.rem(grp, 2)
        wait_all(kv_copies(grp))
        if ahead:
            wait_all(q_copies(grp + Q_AHEAD))
        k_low, v_low = up_project(0, slot)
        kv_low[grp, 0] = k_low
        kv_low[grp, 1] = v_low
        jobs = []
        for head in range(GROUP):
            cols = slice(head * NOPE, (head + 1) * NOPE)
            k_cat = jnp.concatenate([k_low[:, cols], kpe[head % 2, :low_keys]], axis=1)
            jobs.append((queries(grp, head, low), k_cat, v_low[:, cols], cap[:, :low_keys], (low, out_cols(grp, head))))
        attend(jobs, (lambda: q_project(grp + Q_AHEAD)) if ahead else (lambda: None))
        start_all(kv_copies(grp + 2))
        if ahead:
            @pl.when(grp + Q_AHEAD + 2 < groups)
            def _():
                start_all(q_copies(grp + Q_AHEAD + 2))

        @pl.when((grp >= O_AT) & (grp < O_AT + O_SLOTS - 1))
        def _():
            start_all(o_copies(grp - O_AT))

    def low_ahead(grp, _):
        low_step(grp, True)
        return 0

    def low_rest(grp, _):
        low_step(grp, False)
        return 0

    lax.fori_loop(0, groups - Q_AHEAD, low_ahead, 0)
    lax.fori_loop(groups - Q_AHEAD, groups, low_rest, 0)

    def high_step(grp):
        slot = lax.rem(grp, 2)
        wait_all(kv_copies(groups + grp))
        k_up, v_up = up_project(1, slot)
        jobs = []
        for head in range(GROUP):
            cols = slice(head * NOPE, (head + 1) * NOPE)
            keys = jnp.concatenate([kv_low[grp, 0, :, cols], k_up[:, cols]], axis=0)
            values = jnp.concatenate([kv_low[grp, 1, :, cols], v_up[:, cols]], axis=0)
            k_cat = jnp.concatenate([keys, kpe[head % 2]], axis=1)
            jobs.append((queries(grp, head, high), k_cat, values, cap[:, low_keys:], (high, out_cols(grp, head))))
        for first in range(0, GROUP, HIGH_WIDE):
            attend(jobs[first:first + HIGH_WIDE], lambda: None)

        @pl.when(grp + 2 < groups)
        def _():
            start_all(kv_copies(groups + grp + 2))

    depth = (TP - 1 - my_tp, my_tp)
    onward = (left, right)
    back = (right, left)

    def y_slice(side, chunk):
        row, within = chunk // row_chunks, lax.rem(chunk, row_chunks)
        step, part = within // SPLIT, lax.rem(within, SPLIT)
        return (pl.ds(pl.multiple_of(row * PIECE + part * chunk_rows, chunk_rows), chunk_rows),
                pl.ds(pl.multiple_of(side * half_cols + step * COL_BLK, COL_BLK), COL_BLK))

    def f_copy(side, chunk):
        return pltpu.make_async_remote_copy(
            src_ref=acc.at[side, chunk], dst_ref=rbuf.at[side, chunk],
            send_sem=f_send.at[side, chunk], recv_sem=f_recv.at[side, chunk],
            device_id={'tp': onward[side]}, device_id_type=MESH_ID)

    def b_copy(side, chunk):
        part = y_ref.at[y_slice(side, chunk)]
        return pltpu.make_async_remote_copy(
            src_ref=part, dst_ref=part,
            send_sem=b_send.at[side, chunk], recv_sem=b_recv.at[side, chunk],
            device_id={'tp': back[side]}, device_id_type=MESH_ID)

    def y_copy(side, chunk):
        return pltpu.make_async_copy(y_ref.at[y_slice(side, chunk)], y_hbm.at[y_slice(side, chunk)], y_sem.at[side, chunk])

    def reduce_event(side, event, row):
        chunk = event - SUM_LAG * (depth[side] - 1)
        live = (chunk >= 0) & (chunk < row_chunks)
        chunk = chunk + row * row_chunks

        @pl.when(live & (depth[side] > 0))
        def _():
            f_copy(side, chunk).wait_recv()

        @pl.when(live & (depth[side] > 0) & (depth[side] < TP - 1))
        def _():
            acc[side, chunk] = acc[side, chunk] + rbuf[side, chunk]
            f_copy(side, chunk).start()

        @pl.when(live & (depth[side] == TP - 1))
        def _():
            total = acc[side, chunk] + rbuf[side, chunk]
            y_ref[y_slice(side, chunk)] = total.astype(y_ref.dtype)
            b_copy(side, chunk).start()
            y_copy(side, chunk).start()

    def back_event(side, event, row):
        chunk = event - BACK_LAG[row] * (TP - 2 - depth[side])
        live = (chunk >= 0) & (chunk < row_chunks)
        chunk = chunk + row * row_chunks

        @pl.when(live & (depth[side] < TP - 1))
        def _():
            b_copy(side, chunk).wait_recv()

        @pl.when(live & (depth[side] > 0) & (depth[side] < TP - 1))
        def _():
            b_copy(side, chunk).start()

        @pl.when(live & (depth[side] < TP - 1))
        def _():
            y_copy(side, chunk).start()

    def both(event_fn, event, row):
        for part in range(SPLIT):
            for side in range(2):
                event_fn(side, event * SPLIT + part, row)

    def project(row, step):
        turn = row * col_steps + step

        @pl.when(turn + O_SLOTS - 1 < row_blks * col_steps)
        def _():
            start_all(o_copies(turn + O_SLOTS - 1))

        wait_all(o_copies(turn))
        part = jnp.dot(o_ref[row * PIECE:(row + 1) * PIECE], wbig[lax.rem(turn, O_SLOTS), :heads * VALUE], preferred_element_type=jnp.float32)
        for half in range(SPLIT):
            for side in range(2):
                chunk = turn * SPLIT + half
                acc[side, chunk] = part[half * chunk_rows:(half + 1) * chunk_rows, side * COL_BLK:(side + 1) * COL_BLK]

                @pl.when(depth[side] == 0)
                def _():
                    f_copy(side, chunk).start()

    sum_events = pl.cdiv(row_chunks + SUM_LAG * (TP - 2), SPLIT)
    back_events = [pl.cdiv(row_chunks + lag * (TP - 2), SPLIT) for lag in BACK_LAG]

    def low_out(step, _):
        project(0, step)

        @pl.when((step >= LOW_FIRST) & (lax.rem(step, 2) == 0))
        def _():
            both(reduce_event, (step - LOW_FIRST) // 2, 0)
        return 0

    lax.fori_loop(0, col_steps, low_out, 0)

    def high_attention(grp, _):
        high_step(grp)

        @pl.when(lax.rem(grp, 4) != 3)
        def _():
            both(reduce_event, EVENTS_OUT + grp - grp // 4, 0)
        return 0

    lax.fori_loop(0, groups, high_attention, 0)

    first_sum = EVENTS_OUT + groups - groups // 4

    def high_out(step, _):
        project(1, step)

        @pl.when((lax.rem(step, 2) == 0) & (first_sum + step // 2 < sum_events))
        def _():
            both(reduce_event, first_sum + step // 2, 0)

        @pl.when((step >= HIGH_FIRST) & (lax.rem(step, 2) == 1))
        def _():
            both(back_event, (step - HIGH_FIRST) // 2, 0)
        return 0

    lax.fori_loop(0, col_steps, high_out, 0)

    first_back = (col_steps - HIGH_FIRST + 1) // 2

    def high_sum(event, _):
        @pl.when(lax.rem(event, 2) == 1)
        def _():
            both(back_event, first_back + EXTRA + event // 2, 0)

        both(reduce_event, event, 1)
        return 0

    for event in range(first_sum + col_steps // 2, sum_events):
        both(reduce_event, event, 0)
    for event in range(EXTRA):
        both(back_event, first_back + event, 0)
    lax.fori_loop(0, sum_events, high_sum, 0)
    for event in range(first_back + EXTRA + sum_events // 2, back_events[0]):
        both(back_event, event, 0)

    def high_back(event, _):
        both(back_event, event, 1)
        return 0

    lax.fori_loop(0, back_events[1], high_back, 0)

    lat_copy(my_ctx, partner, 0).wait_send()
    lat_copy(my_ctx, across, 1).wait_send()
    lat_copy(across, partner, 2).wait_send()

    def drain(chunk, _):
        for side in range(2):
            @pl.when(depth[side] < TP - 1)
            def _():
                f_copy(side, chunk).wait_send()

            @pl.when(depth[side] > 0)
            def _():
                b_copy(side, chunk).wait_send()

            y_copy(side, chunk).wait()
        return 0

    lax.fori_loop(0, n_chunks, drain, 0)


def store_kernel(src_hbm, dst_hbm, slab, in_sem, out_sem):
    rows = src_hbm.shape[0] // STORE_SLABS
    parts = [pl.ds(part * rows, rows) for part in range(STORE_SLABS)]
    loads = [pltpu.make_async_copy(src_hbm.at[part], slab.at[part], in_sem.at[idx]) for idx, part in enumerate(parts)]
    stores = [pltpu.make_async_copy(slab.at[part], dst_hbm.at[part], out_sem.at[idx]) for idx, part in enumerate(parts)]
    for load in loads:
        load.start()
    for load, store in zip(loads, stores):
        load.wait()
        store.start()
    for store in stores:
        store.wait()


def store_rows(rows):
    hbm = pl.BlockSpec(memory_space=pl.ANY)
    dma = pltpu.SemaphoreType.DMA
    return pl.pallas_call(
        store_kernel,
        out_shape=jax.ShapeDtypeStruct(rows.shape, rows.dtype),
        in_specs=[hbm],
        out_specs=hbm,
        scratch_shapes=[pltpu.VMEM(rows.shape, rows.dtype), dma((STORE_SLABS,)), dma((STORE_SLABS,))],
        name='store_rows',
    )(rows)


def layer(tok_x, tok_pos, w_dq, g_q, w_uq, w_qr, w_dkv, g_kv, w_kr, w_uk, w_uv, w_o):
    n_rows, model_dim = tok_x.shape
    q_rank, lat_rank = w_dq.shape[1], w_dkv.shape[1]
    heads = w_uq.shape[1] // NOPE
    groups = heads // GROUP
    n_keys = CTX * n_rows
    n_chunks = (model_dim // 2 // COL_BLK) * (n_rows // PIECE) * SPLIT
    bf16, f32 = jnp.bfloat16, jnp.float32
    vmem = pl.BlockSpec(memory_space=pltpu.VMEM)
    hbm = pl.BlockSpec(memory_space=pl.ANY)
    dma = pltpu.SemaphoreType.DMA
    y_rows = pl.pallas_call(
        layer_kernel,
        out_shape=jax.ShapeDtypeStruct((n_rows, model_dim), bf16),
        in_specs=[hbm, vmem, vmem, vmem, vmem] + [hbm] * 8,
        out_specs=hbm,
        scratch_shapes=[
            pltpu.VMEM((n_rows, model_dim), bf16),
            pltpu.VMEM((n_rows, model_dim), bf16),
            pltpu.VMEM((ROPE, model_dim), bf16),
            pltpu.VMEM((O_SLOTS, model_dim, DOWN_BLK), bf16),
            pltpu.VMEM((2, q_rank, GROUP * NOPE), bf16),
            pltpu.VMEM((2, q_rank, GROUP * ROPE), bf16),
            pltpu.VMEM((2, 2, lat_rank, GROUP * NOPE), bf16),
            pltpu.VMEM((n_rows, GROUP * ROPE), f32),
            pltpu.VMEM((n_rows, GROUP * ROPE), f32),
            pltpu.VMEM((2, CTX, PIECE, lat_rank + 2 * ROPE), bf16),
            pltpu.VMEM((2, n_keys, 2 * ROPE), bf16),
            pltpu.VMEM((n_rows, q_rank), f32),
            pltpu.VMEM((n_rows, q_rank), bf16),
            pltpu.VMEM((groups, n_rows, GROUP * NOPE), bf16),
            pltpu.VMEM((groups, n_rows, GROUP * ROPE), bf16),
            pltpu.VMEM((groups, 2, n_keys // 2, GROUP * NOPE), bf16),
            pltpu.VMEM((PIECE, n_keys // 2 + n_keys), f32),
            pltpu.VMEM((n_rows, heads * VALUE), bf16),
            pltpu.VMEM((2, n_chunks, PIECE // SPLIT, COL_BLK), f32),
            pltpu.VMEM((2, n_chunks, PIECE // SPLIT, COL_BLK), f32),
            dma, dma, dma((O_SLOTS,)), dma((2, 2)), dma((2, 2)), dma((O_SLOTS, 2)),
            dma((3,)), dma((3,)),
            dma((2, n_chunks)), dma((2, n_chunks)), dma((2, n_chunks)), dma((2, n_chunks)), dma((2, n_chunks)),
        ],
        compiler_params=pltpu.CompilerParams(collective_id=0, has_side_effects=True, vmem_limit_bytes=67043328),
        name='layer',
    )(tok_x, tok_pos, jnp.asarray(inv_freq_row()), g_q, g_kv, w_dq, w_uq, w_qr, w_dkv, w_kr.T, w_uk, w_uv, w_o)
    return store_rows(y_rows)


def solution(mesh):
    tok_spec = P(('dp', 'ctx'), None)
    pos_spec = P(('dp', 'ctx'))
    full_mat = P(None, None)
    full_vec = P(None)
    col_spec = P(None, 'tp')
    row_spec = P('tp', None)
    return jax.shard_map(layer, mesh=mesh,
                         in_specs=(tok_spec, pos_spec, full_mat, full_vec, col_spec, col_spec, full_mat, full_vec, full_mat, col_spec, col_spec, row_spec),
                         out_specs=tok_spec, check_vma=False)
```
